128 devices in a mesh: tm: 8 (over y, core), lat: 16 (over x, z).
Axes of the slice: x: 4, y: 4, z: 4, core: 2. Of those that a mesh axis runs over, the one named last changes fastest.
Arguments:
- trajectory: float32 [8, 64, 64, 2048], P('tm', 'lat'), may hold values from -6 to 6
- diffusivity: float32 [8, 64, 64, 2048], P('tm', 'lat'), may hold values from 0.02 to 0.24
- adjoint_end: bfloat16 [64, 64, 2048], P('lat'), may hold values from -6 to 6
- obs_jac: bfloat16 [12288, 128, 128], P(('tm', 'lat')), may hold values from -0.5 to 0.5
- obs_value: float32 [12288, 128], P(('tm', 'lat')), may hold values from -6 to 6
- obs_weight: float32 [12288, 128], P(('tm', 'lat')), may hold values from 0.3 to 3
- obs_valid: int32 [12288, 128], P(('tm', 'lat')), may hold values 0 or 1
- obs_owner: int32 [12288, 1], P(('tm', 'lat')), may hold values from 0 to 127; in each aligned block of 96 rows (0 to 95, 96 to 191, ...) at most 2 rows name the same one
- obs_tile: int32 [12288], P(('tm', 'lat')), may hold values from 0 to 4095
Outputs:
- adjoint: float32 [8, 64, 64, 2048], P('tm', 'lat')
The draws below stay inside these ranges and needn't reach their ends.
Inputs may be any that keep to these rules, and one draw needn't show every extreme that they name: `obs_owner`: among the 96 blocks of one device, no owner is named more than 2 times, a bound that some block reaches.
All inputs are finite; a program needn't handle non-finite values. No bound on the sum of `obs_valid` on one device may be relied on, other than what follows from the above.
Results may differ from the reference program's by a relative error of at most 0.0024.
Values may be sent and summed in bfloat16 or wider, within the bound.
A program may use at most 128 MiB of HBM per device.

```python
import math
import jax
import jax.numpy as jnp
import numpy as np
from jax import lax

NLON = 2048
LEV = 64
TW = 2
CH = 128
SUB = 2
NB_DEV = 96
SECTIONS = 8
NLAT = 64
TILE = 128
TILES_DEV = 4096
CAP = 2
NOBS = 12288
N_LAT = 16
DEVICES = 128


def with_ends(entries, key, smallest, high):
    shape = entries.shape
    place = [jax.random.randint(jax.random.fold_in(key, axis), (), 0, shape[axis]) for axis in range(len(shape))]
    entries = entries.at[tuple(place)].set(smallest)
    longest = shape.index(max(shape))
    place[longest] = (place[longest] + 1) % shape[longest]
    return entries.at[tuple(place)].set(high)


def block_levels(rng, shape, cuts, least, largest):
    def one(dim, parts):
        draws = jax.random.uniform(jax.random.fold_in(jax.random.fold_in(rng, 6), dim), (parts,), jnp.float32, least / len(cuts), largest / len(cuts))
        return jnp.repeat(jnp.exp(draws), shape[dim] // parts).reshape((-1,) + (1,) * (len(shape) - dim - 1))

    loudness = one(*cuts[0])
    for cut in cuts[1:]:
        loudness = loudness * one(*cut)
    return loudness


def deal_out(key, own, number, rows, count, top, most, lean):
    sequence = jax.random.permutation(key, count)
    packed, ordinary = load_shares(count, rows * top, most, lean, True), load_shares(count, rows * top, most, lean, False)
    places = jnp.arange(count)

    def named(tallies, rotation):
        used = int((tallies > 0).sum())
        fixed = max(1, used // 4)
        shifted = fixed + (places - fixed + rotation * (used - fixed)) % max(1, count - fixed)
        return jnp.zeros((count,), jnp.int32).at[sequence[jnp.where(places < fixed, places, shifted)]].set(jnp.asarray(tallies, jnp.int32))

    tallies = jnp.where(number % 4 == 0, named(packed, number // 4), named(ordinary, number - number // 4 - 1))
    mixed = jax.random.permutation(jax.random.fold_in(own, 3), count)
    source_of, sink = mixed[0:count // 2 * 2:2], mixed[1:count // 2 * 2:2]
    slack = jnp.minimum(tallies[source_of] - 1, most - tallies[sink]) // 2
    slack = jnp.where((source_of == sequence[0]) | (sink == sequence[0]) | (tallies[sink] == 0), 0, jnp.maximum(slack, 0))
    shifted = jax.random.randint(jax.random.fold_in(own, 4), (count // 2,), 0, 1 << 20) % (slack + 1)
    tallies = tallies.at[source_of].add(-shifted).at[sink].add(shifted)
    labels = jnp.searchsorted(jnp.cumsum(tallies), jnp.arange(rows * top), side="right").astype(jnp.int32)
    grid = labels.reshape(top, rows).T
    grid = grid[jax.random.permutation(jax.random.fold_in(own, 1), rows)]
    rotation = jax.random.randint(jax.random.fold_in(own, 2), (rows, 1), 0, top)
    return jnp.take_along_axis(grid, (jnp.arange(top)[None, :] + rotation) % top, axis=1)


def load_shares(amount, total, most, slope, full):
    weights = [(1 << 20) // math.isqrt(standing ** slope) + 1 for standing in range(1, amount + 1)]
    largest = most if full else min(most, max(-(-total // amount), total * weights[0] // sum(weights)))
    least = 1 if total - largest >= amount - 1 else 0
    counts, surplus = [largest] + [least] * (amount - 1), total - largest - least * (amount - 1)
    while surplus > 0:
        movable = [i for i in range(1, amount) if counts[i] < largest] or [i for i in range(1, amount) if counts[i] < most]
        mass, remaining = sum([weights[i] for i in movable]), surplus
        for i in movable:
            more = min(most - counts[i], max(1, remaining * weights[i] // mass), surplus)
            counts[i] = counts[i] + more
            surplus = surplus - more
    return np.array(counts)


def gaussian(rng, shape, scale, most, shards=(), held_as=jnp.bfloat16):
    level = block_levels(rng, shape, shards, -0.22, 0.18) if shards else 1.0
    result = jax.random.normal(rng, shape, jnp.float32) * scale * level
    return jnp.minimum(jnp.maximum(result, -most), most).astype(held_as)


def setup_inputs(seed: int = 0) -> dict:
    streams_of = jax.random.split(jax.random.key(seed), 10)
    trajectory = gaussian(streams_of[0], (SECTIONS, NLAT, LEV, NLON), 1.0, 6.0, ((0, 8), (1, 16)), jnp.float32)
    diffusivity = jnp.clip(jnp.exp(math.log(0.24) - 2.4849066 * jax.random.uniform(streams_of[1], (SECTIONS, NLAT, LEV, NLON), jnp.float32) ** block_levels(streams_of[1], (SECTIONS, NLAT, LEV, NLON), ((0, 8), (1, 16)), -0.2, 0.2)), 0.02, 0.24)
    adjoint_end = gaussian(streams_of[2], (NLAT, LEV, NLON), 1.0, 6.0, ((0, 16),))
    obs_jac = gaussian(streams_of[3], (NOBS, CH, TILE), TILE ** -0.5, 0.5, ((0, 128),))
    obs_value = gaussian(streams_of[4], (NOBS, CH), 1.0, 6.0, ((0, 128),), jnp.float32)
    obs_weight = jnp.clip(jnp.exp(math.log(3.0) - 2.3025851 * jax.random.uniform(streams_of[5], (NOBS, CH), jnp.float32) ** block_levels(streams_of[5], (NOBS, CH), ((0, 128),), -0.2, 0.2)), 0.3, 3.0)
    obs_valid = with_ends((jax.random.randint(streams_of[6], (NOBS, CH), 0, 4) < 3).astype(jnp.int32), jax.random.fold_in(streams_of[6], 1), 0, 1)
    obs_owner_keys = jax.random.split(jax.random.fold_in(streams_of[7], 1), NOBS // NB_DEV)
    obs_owner_turns = jax.random.permutation(jax.random.fold_in(streams_of[7], 3), NOBS // NB_DEV)
    obs_owner = jax.vmap(lambda own, number: deal_out(jax.random.fold_in(streams_of[7], 2), own, number, NB_DEV, DEVICES, 1, CAP, 2))(obs_owner_keys, obs_owner_turns).reshape((NOBS, 1))
    obs_tile = with_ends(jax.random.randint(streams_of[8], (NOBS,), 0, TILES_DEV), jax.random.fold_in(streams_of[8], 1), 0, TILES_DEV - 1).astype(jnp.int32)
    return dict(trajectory=trajectory, diffusivity=diffusivity, adjoint_end=adjoint_end, obs_jac=obs_jac, obs_value=obs_value, obs_weight=obs_weight, obs_valid=obs_valid, obs_owner=obs_owner, obs_tile=obs_tile)


def spread(weighted):
    padded = jnp.pad(weighted, ((1, 1), (0, 0), (0, 0)))
    return padded[2:] + padded[:-2] + jnp.roll(weighted, 1, 2) + jnp.roll(weighted, -1, 2) - 4.0 * weighted


def propagate(field, kappa):
    for _ in range(SUB):
        field = field + spread(kappa * field)
    return field


def reference(trajectory, diffusivity, adjoint_end, obs_jac, obs_value, obs_weight, obs_valid, obs_owner, obs_tile):
    per_row = NLON // TW
    tiles = trajectory.reshape(SECTIONS, NLAT, LEV, per_row, TW).transpose(0, 1, 3, 2, 4).reshape(SECTIONS * NLAT * per_row, TILE)
    owner = obs_owner[:, 0]
    section = owner // N_LAT
    band = owner % N_LAT
    flat = (section * NLAT * per_row + band * TILES_DEV + obs_tile).astype(jnp.int32)
    states = tiles[flat]
    weights = obs_weight * obs_valid.astype(jnp.float32)

    def one(args):
        jac, state, value, weight = args
        jac_f = jac.astype(jnp.float32)
        pred = jnp.einsum("bct,bt->bc", jac_f, state, precision=lax.Precision.HIGHEST)
        resid = weight * (value - pred)
        return jnp.einsum("bct,bc->bt", jac_f, resid, precision=lax.Precision.HIGHEST)

    terms = lax.map(one, (obs_jac.reshape(DEVICES, NB_DEV, CH, TILE), states.reshape(DEVICES, NB_DEV, TILE),
                          obs_value.reshape(DEVICES, NB_DEV, CH), weights.reshape(DEVICES, NB_DEV, CH)))
    terms = terms.reshape(NOBS, TILE)
    forcing = jnp.zeros((SECTIONS * NLAT * per_row, TILE), jnp.float32).at[flat].add(terms)
    forcing = forcing.reshape(SECTIONS, NLAT, per_row, LEV, TW).transpose(0, 1, 3, 2, 4).reshape(SECTIONS, NLAT, LEV, NLON)
    results = [None] * SECTIONS
    current = adjoint_end.astype(jnp.float32)
    for section_id in range(SECTIONS - 1, -1, -1):
        if section_id == SECTIONS - 1:
            incoming = adjoint_end.astype(jnp.float32)
        else:
            incoming = lax.optimization_barrier(current.astype(jnp.bfloat16)).astype(jnp.float32)
        current = forcing[section_id] + propagate(incoming, diffusivity[section_id])
        results[section_id] = current
    return jnp.stack(results)
```

```python
import jax
import jax.numpy as jnp
from jax import lax
from jax.experimental import pallas as pl
from jax.experimental.pallas import tpu as pltpu
from jax.sharding import PartitionSpec as P

f32, bf16, i16, i32 = jnp.float32, jnp.bfloat16, jnp.int16, jnp.int32
MESH = pl.DeviceIdType.MESH

DEV = 128
NB = 96
BANDS = 12
CHUNK = 64
KMID, KSCALE = 0.13, 0.11 / 32700.0


def split(x):
    hi = x.astype(bf16)
    return hi, (x - hi.astype(f32)).astype(bf16)


def dot(a, b, ca, cb):
    return lax.dot_general(a, b, (((ca,), (cb,)), ((), ())), preferred_element_type=f32)


def iota(shape, dim):
    return lax.broadcasted_iota(i32, shape, dim)


def kernel(
    traj_ref, kap_ref, end_ref, jac_ref, val_ref, wgt_ref, vld_ref, own_ref, til_ref,
    out_ref,
    TRJ, KIN, EIN, JAC, E32,
    AS, AR, TT, LOH, ACC, BS, BR, S3, PR, CS, CR, RT,
    KS, KR, ES, EN, W, WT, OS, OR,
    lsem, asem, bsem, csem, ksend, krecv, esem, osem,
):
    tm = lax.axis_index("tm")
    lat = lax.axis_index("lat")
    me = tm * 16 + lat
    half = lax.rem(tm, 2)
    pair = lax.div(tm, 2)
    level = pair * 16 + lat
    lb_me = lat - 4 * half
    in_me = (lb_me >= 0) & (lb_me < BANDS)

    loads = [
        pltpu.make_async_copy(traj_ref, TRJ, lsem.at[0]),
        pltpu.make_async_copy(jac_ref, JAC, lsem.at[1]),
        pltpu.make_async_copy(
            end_ref.at[:, pl.ds(pl.multiple_of(pair * 16, 16), 16), :], EIN, lsem.at[2]
        ),
    ]
    for h in range(16):
        loads.append(
            pltpu.make_async_copy(
                kap_ref.at[:, :, pl.ds(h * 128, 128)], KIN.at[h], lsem.at[3 + h]
            )
        )
    for copy in loads:
        copy.start()

    own = own_ref[...]
    eye = iota((NB, NB), 0) == iota((NB, NB), 1)
    own_row = jnp.sum(jnp.where(eye, own.astype(f32), 0.0), axis=0, keepdims=True)
    til = jnp.sum(jnp.where(eye, til_ref[...].astype(f32), 0.0), axis=1, keepdims=True)
    same = (own.astype(f32) == own_row) & (iota((NB, NB), 1) < iota((NB, NB), 0))
    rank = jnp.sum(jnp.where(same, 1.0, 0.0), axis=1, keepdims=True).astype(i32)
    place = rank * DEV + own
    hit = iota((NB, 2 * DEV), 1) == place
    M = jnp.where(hit, 1.0, 0.0).astype(bf16)
    ids = jnp.sum(jnp.where(hit, til + 1.0, 0.0), axis=0, keepdims=True)
    AS[0, 0:1, :] = ids[:, :DEV]
    AS[0, 1:2, :] = ids[:, DEV:]
    AR[me] = AS[0]

    def peers(fn):
        def step(i, carry):
            d = lax.rem(me + i, DEV)
            fn(d, lax.div(d, 16), lax.rem(d, 16))
            return carry

        lax.fori_loop(1, DEV, step, 0)

    def send_a(d, t, l):
        pltpu.make_async_remote_copy(
            AS.at[0], AR.at[me], asem.at[0], asem.at[1], device_id=(t, l), device_id_type=MESH
        ).start()

    peers(send_a)

    loads[2].wait()
    for h in range(16):
        E32[h] = EIN[:, :, h * 128 : (h + 1) * 128].astype(f32)
    e2 = E32.reshape(16 * 4 * 16, 128)

    def end_level(l, carry):
        for r in range(4):
            ES[l, r * 16 : (r + 1) * 16, :] = e2[pl.ds(r * 16 + l, 16, stride=64), :].astype(bf16)
        return carry

    lax.fori_loop(0, 16, end_level, 0)

    @pl.when(in_me)
    def _():
        EN[lb_me] = ES[lat]

        def send_e(i, carry):
            l = lax.rem(lat + i, 16)
            pltpu.make_async_remote_copy(
                ES.at[l], EN.at[lb_me], esem.at[0], esem.at[1], device_id=(tm, l), device_id_type=MESH
            ).start()
            return carry

        lax.fori_loop(1, 16, send_e, 0)

    for copy in loads[3:]:
        copy.wait()
    k2 = KIN.reshape(16 * 4 * 64, 128)

    def kap_level(l, carry):
        for r in range(4):
            k = k2[pl.ds(r * 64 + l, 16, stride=256), :]
            q = jnp.round((k - KMID) * (1.0 / KSCALE))
            KS[l, r * 16 : (r + 1) * 16, :] = q.astype(i32).astype(i16)
        return carry

    lax.fori_loop(0, 64, kap_level, 0)

    def send_k(d, t, l):
        c = lax.rem(t, 2)
        lb = lat - 4 * c

        @pl.when((lb >= 0) & (lb < BANDS))
        def _():
            pltpu.make_async_remote_copy(
                KS.at[lax.div(t, 2) * 16 + l], KR.at[tm * BANDS + lb], ksend.at[c], krecv,
                device_id=(t, l), device_id_type=MESH,
            ).start()

    peers(send_k)

    @pl.when(in_me)
    def _():
        KR[tm * BANDS + lb_me] = KS[level]

    def wait_n(buf, n, sem):
        part = buf.at[pl.ds(0, n)]
        pltpu.make_async_copy(part, part, sem).wait()

    wait_n(AR, DEV - 1, asem.at[1])
    for s in range(2):
        TT[s] = AR[:, s, :].T
    tid = jnp.concatenate([TT[s, pl.ds(me, 1), :] for s in range(2)], axis=1).astype(i32) - 1
    low = (tid & 127) * 2
    group = jnp.concatenate([tid >> 7, tid >> 7], axis=1)
    LOH[...] = jnp.where(
        iota((256, 512), 0) == jnp.concatenate([low, low + 1], axis=1), 1.0, 0.0
    ).astype(bf16)
    ACC[...] = jnp.zeros((64, 512), f32)
    loads[0].wait()

    def gather_row(r, carry):
        total = ACC[...]
        for g in range(8):
            hi, lo = split(TRJ[r, :, g * 256 : (g + 1) * 256])
            y = dot(jnp.concatenate([hi, lo], axis=0), LOH[...], 1, 0)
            total = total + jnp.where(group == r * 8 + g, y[:64] + y[64:], 0.0)
        ACC[...] = total
        return carry

    lax.fori_loop(0, 4, gather_row, 0)
    for s in range(2):
        x = jnp.concatenate(
            [ACC[:, s * 128 : (s + 1) * 128], ACC[:, 256 + s * 128 : 256 + (s + 1) * 128]], axis=0
        )
        BS[:, s, :] = x.T
    BR[me] = BS[me]

    def send_b(d, t, l):
        pltpu.make_async_remote_copy(
            BS.at[d], BR.at[me], bsem.at[0], bsem.at[1], device_id=(t, l), device_id_type=MESH
        ).start()

    peers(send_b)

    S3[...] = jnp.zeros((NB, 8, 128), f32)
    swap = jnp.where(
        iota((128, 128), 1) == (iota((128, 128), 0) & 63) * 2 + (iota((128, 128), 0) >> 6), 1.0, 0.0
    ).astype(bf16)
    wait_n(BR, DEV - 1, bsem.at[1])
    parts = [split(BR[:, s, :]) for s in range(2)]
    for p in range(2):
        mine = dot(M[:, :DEV], parts[0][p], 1, 0) + dot(M[:, DEV:], parts[1][p], 1, 0)
        S3[:, p, :] = dot(mine.astype(bf16), swap, 1, 0)
    loads[1].wait()

    def predict(b, carry):
        PR[b] = dot(S3[b].astype(bf16), JAC[b], 1, 1)
        return carry

    lax.fori_loop(0, NB, predict, 0, unroll=8)
    weight = wgt_ref[...] * vld_ref[...].astype(f32)
    resid = weight * (val_ref[...] - (PR[:, 0, :] + PR[:, 1, :]))
    for p, part in enumerate(split(resid)):
        S3[:, p, :] = part.astype(f32)

    def adjoin(b, carry):
        PR[b] = dot(S3[b].astype(bf16), JAC[b], 1, 0)
        return carry

    lax.fori_loop(0, NB, adjoin, 0, unroll=8)
    placed = jnp.zeros((128, 256), f32)
    for part in split(PR[:, 0, :] + PR[:, 1, :]):
        placed = placed + dot(dot(part, swap, 1, 1).astype(bf16), M, 0, 0)
    for s in range(2):
        for w in range(2):
            CS[:, s * 2 + w, :] = placed[w * 64 : (w + 1) * 64, s * 128 : (s + 1) * 128]
    CR[me] = CS[level]

    def send_c(d, t, l):
        pltpu.make_async_remote_copy(
            CS.at[lax.div(t, 2) * 16 + l], CR.at[me], csem.at[0], csem.at[1],
            device_id=(t, l), device_id_type=MESH,
        ).start()

    peers(send_c)

    @pl.when(in_me)
    def _():
        wait_n(EN, BANDS - 1, esem.at[1])
        wait_n(KR, 8 * BANDS - 1, krecv)

    @pl.when(jnp.logical_not(in_me))
    def _():
        wait_n(EN, BANDS, esem.at[1])
        wait_n(KR, 8 * BANDS, krecv)

    for lb in range(BANDS):
        W[lb * 4 : lb * 4 + 4] = EN[lb].astype(f32).reshape(4, 16, 128)
    WT[0] = jnp.zeros((16, 128), f32)
    WT[49] = jnp.zeros((16, 128), f32)
    lane = iota((8, 16, 128), 2)

    def substeps(s):
        def one(_, carry):
            for g in range(6):
                k = KR[pl.ds(s * BANDS + g * 2, 2)].astype(i32).astype(f32) * KSCALE + KMID
                WT[1 + g * 8 : 9 + g * 8] = k.reshape(8, 16, 128) * W[g * 8 : g * 8 + 8]
            for g in range(6):
                x = WT[1 + g * 8 : 9 + g * 8]
                a = pltpu.roll(x, 1, axis=2)
                b = pltpu.roll(x, 127, axis=2)
                a = jnp.where(lane == 0, pltpu.roll(a, 1, axis=1), a)
                b = jnp.where(lane == 127, pltpu.roll(b, 15, axis=1), b)
                sides = (WT[2 + g * 8 : 10 + g * 8] + WT[g * 8 : g * 8 + 8]) + (a + b)
                W[g * 8 : g * 8 + 8] = W[g * 8 : g * 8 + 8] + (sides - 4.0 * x)
            return carry

        lax.fori_loop(0, 2, one, 0)

    def finish(s):
        def band(lb, carry):
            o = s * 16 + lb + 4 * half
            tid = jnp.concatenate([TT[k, pl.ds(o, 1), :] for k in range(2)], axis=1).astype(i32) - 1
            low = (tid & 63) * 2
            right = jnp.where(
                iota((128, 512), 0) == jnp.concatenate([low, low + 1], axis=1), 1.0, 0.0
            ).astype(bf16)
            mask = iota((64, 256), 0) == (tid >> 6)
            left = []
            for w in range(2):
                term = jnp.concatenate([RT[k * 2 + w, pl.ds(o, 1), :] for k in range(2)], axis=1)
                left.append([jnp.where(mask, p.astype(f32), 0.0).astype(bf16) for p in split(term)])
            lhs = jnp.concatenate(
                [jnp.concatenate([left[0][p], left[1][p]], axis=1) for p in range(2)], axis=0
            )
            y = dot(lhs, right, 1, 1)
            rows = pl.ds(lb * 4, 4)
            W[rows] = W[rows] + (y[:64] + y[64:]).reshape(4, 16, 128)
            return carry

        lax.fori_loop(0, BANDS, band, 0)

        def deliver(j, carry):
            OS[s * 8 + j] = W[pl.ds(half * 16 + j * 4, 4)].reshape(CHUNK, 128).astype(bf16)
            to = half * 8 + j

            @pl.when((s == tm) & (to == lat))
            def _():
                OR[level] = OS[s * 8 + j]

            @pl.when((s != tm) | (to != lat))
            def _():
                pltpu.make_async_remote_copy(
                    OS.at[s * 8 + j], OR.at[level], osem.at[0], osem.at[1],
                    device_id=(s, to), device_id_type=MESH,
                ).start()

            return carry

        lax.fori_loop(0, 8, deliver, 0)

    substeps(7)
    wait_n(CR, DEV - 1, csem.at[1])
    for q in range(4):
        RT[q] = CR[:, q, :].T

    def section(i, carry):
        s = 7 - i
        finish(s)
        W[...] = W[...].astype(bf16).astype(f32)
        substeps(s - 1)
        return carry

    lax.fori_loop(0, 7, section, 0)
    finish(0)

    mine_o = lax.div(lat, 8) == half

    @pl.when(mine_o)
    def _():
        wait_n(OR, 63, osem.at[1])

    @pl.when(jnp.logical_not(mine_o))
    def _():
        wait_n(OR, 64, osem.at[1])

    def store(l, carry):
        for r in range(4):
            out_ref[pl.ds(r * 64 + l, 16, stride=256), :] = OR[l, r * 16 : (r + 1) * 16, :].astype(f32)
        return carry

    lax.fori_loop(0, 64, store, 0)

    wait_n(AR, DEV - 1, asem.at[0])
    wait_n(BS, DEV - 1, bsem.at[0])
    wait_n(CR, DEV - 1, csem.at[0])

    @pl.when(in_me)
    def _():
        wait_n(ES, 15, esem.at[0])

    for c in range(2):
        inside = (lat < BANDS) if c == 0 else (lat >= 4)

        @pl.when(inside & (half == c))
        def _():
            wait_n(KS, 63, ksend.at[c])

        @pl.when(inside & (half != c))
        def _():
            wait_n(KS, 64, ksend.at[c])

    @pl.when(mine_o)
    def _():
        wait_n(OS, 63, osem.at[0])

    @pl.when(jnp.logical_not(mine_o))
    def _():
        wait_n(OS, 64, osem.at[0])


def per_device(traj, kap, end, jac, val, wgt, vld, own, til):
    hbm = pl.BlockSpec(memory_space=pl.ANY)
    vmem = pl.BlockSpec(memory_space=pltpu.VMEM)
    dma = pltpu.SemaphoreType.DMA
    V = pltpu.VMEM
    out = pl.pallas_call(
        kernel,
        out_shape=jax.ShapeDtypeStruct((16 * 4 * 64, 128), f32),
        in_specs=[hbm] * 4 + [vmem] * 5,
        out_specs=vmem,
        scratch_shapes=[
            V((4, 64, 2048), f32), V((16, 4, 64, 128), f32), V((4, 16, 2048), bf16),
            V((NB, 128, 128), bf16), V((16, 4, 16, 128), f32),
            V((1, 2, 128), f32), V((DEV, 2, 128), f32), V((2, 128, 128), f32),
            V((256, 512), bf16), V((64, 512), f32), V((DEV, 2, 128), f32), V((DEV, 2, 128), f32),
            V((NB, 8, 128), f32), V((NB, 8, 128), f32), V((64, 4, 128), f32), V((DEV, 4, 128), f32),
            V((4, 128, 128), f32),
            V((64, CHUNK, 128), i16), V((8 * BANDS, CHUNK, 128), i16),
            V((16, CHUNK, 128), bf16), V((BANDS, CHUNK, 128), bf16),
            V((48, 16, 128), f32), V((50, 16, 128), f32),
            V((64, CHUNK, 128), bf16), V((64, CHUNK, 128), bf16),
            dma((19,)), dma((2,)), dma((2,)), dma((2,)), dma((2,)), dma, dma((2,)), dma((2,)),
        ],
        compiler_params=pltpu.CompilerParams(has_side_effects=True, vmem_limit_bytes=56 << 20),
        name="adjoint_sweep",
    )(traj[0], kap[0], end, jac, val, wgt, vld, own, til.reshape(1, NB))
    return out.reshape(16, 4, 64, 128).transpose(1, 2, 0, 3).reshape(1, 4, 64, 2048)


def solution(mesh):
    both = ("tm", "lat")
    in_specs = (
        P("tm", "lat", None, None),
        P("tm", "lat", None, None),
        P("lat", None, None),
        P(both, None, None),
        P(both, None),
        P(both, None),
        P(both, None),
        P(both, None),
        P(both),
    )
    return jax.shard_map(
        per_device, mesh=mesh, in_specs=in_specs, out_specs=P("tm", "lat", None, None),
        check_vma=False,
    )
```

```python
import jax
import jax.numpy as jnp
from jax import lax
from jax.experimental import pallas as pl
from jax.experimental.pallas import tpu as pltpu
from jax.sharding import PartitionSpec as P

f32, bf16, i16, i32 = jnp.float32, jnp.bfloat16, jnp.int16, jnp.int32
MESH = pl.DeviceIdType.MESH

DEV = 128
NB = 96
BANDS = 12
KFIRST = 32
CHUNK = 64
KMID, KSCALE = 0.13, 0.11 / 32700.0


def split(x):
    hi = x.astype(bf16)
    return hi, (x - hi.astype(f32)).astype(bf16)


def dot(a, b, ca, cb):
    return lax.dot_general(a, b, (((ca,), (cb,)), ((), ())), preferred_element_type=f32)


def iota(shape, dim):
    return lax.broadcasted_iota(i32, shape, dim)


def kernel(
    traj_ref, kap_ref, end_ref, jac_ref, val_ref, wgt_ref, vld_ref, own_ref, til_ref,
    out_ref,
    TRJ, KIN, KQ, EIN, EQ, JAC,
    AS, AR, TT, LOH, ACC, BS, BR, S3, PR, CS, CR, RT, OHR,
    KS, KR, ES, EN, W, WT, KF, OS, OR,
    lsem, asem, bsem, csem, ksem, esem, fsem, osem,
):
    tm = lax.axis_index("tm")
    lat = lax.axis_index("lat")
    me = tm * 16 + lat
    half = lax.rem(tm, 2)
    pair = lax.div(tm, 2)
    level = pair * 16 + lat
    mate = tm + 1 - 2 * half
    side = lax.div(lat, 8)
    home = side == half
    away = side != half

    def peers(fn):
        def step(i, carry):
            d = lax.rem(me + i, DEV)
            fn(d, lax.div(d, 16), lax.rem(d, 16))
            return carry

        lax.fori_loop(1, DEV, step, 0)

    def send(src, dst, sems, t, l):
        return pltpu.make_async_remote_copy(
            src, dst, sems.at[0], sems.at[1], device_id=(t, l), device_id_type=MESH
        )

    def wait_n(buf, n, sem):
        part = buf.at[pl.ds(0, n)]
        pltpu.make_async_copy(part, part, sem).wait()

    def wait_home(buf, n, sem):
        @pl.when(home)
        def _():
            wait_n(buf, n - 1, sem)

        @pl.when(away)
        def _():
            wait_n(buf, n, sem)

    loads = [
        pltpu.make_async_copy(kap_ref, KIN, lsem.at[0]),
        pltpu.make_async_copy(
            end_ref.at[:, pl.ds(pl.multiple_of(pair * 16, 16), 16), :], EIN, lsem.at[1]
        ),
        pltpu.make_async_copy(traj_ref, TRJ, lsem.at[2]),
        pltpu.make_async_copy(jac_ref, JAC, lsem.at[3]),
    ]
    for copy in loads:
        copy.start()
    barrier = pltpu.get_barrier_semaphore()
    peers(
        lambda d, t, l: pl.semaphore_signal(barrier, 1, device_id=(t, l), device_id_type=MESH)
    )

    eye = iota((NB, NB), 0) == iota((NB, NB), 1)
    own_row = own_ref[...].astype(f32)
    own = jnp.sum(jnp.where(eye, own_row, 0.0), axis=1, keepdims=True)
    til = jnp.sum(jnp.where(eye, til_ref[...].astype(f32), 0.0), axis=1, keepdims=True)
    same = (own == own_row) & (iota((NB, NB), 1) < iota((NB, NB), 0))
    rank = jnp.sum(jnp.where(same, 1.0, 0.0), axis=1, keepdims=True)
    hit = iota((NB, 2 * DEV), 1) == (rank * DEV + own).astype(i32)
    M = jnp.where(hit, 1.0, 0.0).astype(bf16)
    ids = jnp.sum(jnp.where(hit, til + 1.0, 0.0), axis=0, keepdims=True)
    AS[0, 0:1, :] = ids[:, :DEV]
    AS[0, 1:2, :] = ids[:, DEV:]
    AR[me] = AS[0]

    apart = jnp.where(
        iota((256, 256), 0) == (iota((256, 256), 1) & 127) * 2 + (iota((256, 256), 1) >> 7), 1.0, 0.0
    ).astype(bf16)

    loads[0].wait()

    def kap_row(r, carry):
        for g in range(8):
            q = jnp.round((KIN[r, :, g * 256 : (g + 1) * 256] - KMID) * (1.0 / KSCALE))
            a = jnp.round(q * (1.0 / 256.0))
            b = q - a * 256.0
            y = dot(jnp.concatenate([a, b], axis=0).astype(bf16), apart, 1, 0)
            y = y[:64] * 256.0 + y[64:]
            rows = pl.ds(pl.multiple_of(r * 64, 64), 64)
            KQ[g, rows, :] = y[:, :128]
            KQ[8 + g, rows, :] = y[:, 128:]
        return carry

    lax.fori_loop(0, 4, kap_row, 0)
    k2 = KQ.reshape(16 * 256, 128)

    def kap_level(l, carry):
        for r in range(4):
            q = k2[pl.ds(r * 64 + l, 16, stride=256), :]
            KS[l, r * 16 : (r + 1) * 16, :] = q.astype(i32).astype(i16)
        return carry

    lax.fori_loop(0, 64, kap_level, 0, unroll=2)

    loads[1].wait()
    for r in range(4):
        for g in range(8):
            y = dot(EIN[r, :, g * 256 : (g + 1) * 256], apart, 1, 0)
            EQ[g, r * 16 : (r + 1) * 16, :] = y[:, :128]
            EQ[8 + g, r * 16 : (r + 1) * 16, :] = y[:, 128:]
    e2 = EQ.reshape(16 * 64, 128)

    def end_level(l, carry):
        for r in range(4):
            rows = e2[pl.ds(r * 16 + half * 8 + l, 16, stride=64), :]
            ES[l, r * 16 : (r + 1) * 16, :] = rows.astype(bf16)
        return carry

    lax.fori_loop(0, 8, end_level, 0)
    lb_me = lat - 4 * side

    @pl.when(home)
    def _():
        KR[lb_me * 8 + tm] = KS[level]
        EN[lb_me] = ES[lat - 8 * half]

    pl.semaphore_wait(barrier, DEV - 1)
    peers(lambda d, t, l: send(AS.at[0], AR.at[me], asem, t, l).start())

    def send_k(lo, hi):
        def step(i, carry):
            l = lax.rem(level + i * 27, 64)

            @pl.when((i > 0) | away)
            def _():
                send(
                    KS.at[l], KR.at[lb_me * 8 + tm], ksem, lax.div(l, 16) * 2 + side, lax.rem(l, 16)
                ).start()

            return carry

        lax.fori_loop(lo, hi, step, 0)

    def send_e(i, carry):
        l = half * 8 + i

        @pl.when((l != lat) | away)
        def _():
            send(ES.at[i], EN.at[lb_me], esem, pair * 2 + side, l).start()

        return carry

    send_k(0, KFIRST)

    wait_n(AR, DEV - 1, asem.at[1])
    for s in range(2):
        TT[s] = AR[:, s, :].T
    tid = jnp.concatenate([TT[s, pl.ds(me, 1), :] for s in range(2)], axis=1).astype(i32) - 1
    low = (tid & 127) * 2
    group = jnp.concatenate([tid >> 7, tid >> 7], axis=1)
    LOH[...] = jnp.where(
        iota((256, 512), 0) == jnp.concatenate([low, low + 1], axis=1), 1.0, 0.0
    ).astype(bf16)
    ACC[...] = jnp.zeros((64, 512), f32)
    loads[2].wait()

    def gather_row(r, carry):
        total = ACC[...]
        for g in range(8):
            hi, lo = split(TRJ[r, :, g * 256 : (g + 1) * 256])
            y = dot(jnp.concatenate([hi, lo], axis=0), LOH[...], 1, 0)
            total = total + jnp.where(group == r * 8 + g, y[:64] + y[64:], 0.0)
        ACC[...] = total
        return carry

    lax.fori_loop(0, 4, gather_row, 0)
    for s in range(2):
        x = jnp.concatenate(
            [ACC[:, s * 128 : (s + 1) * 128], ACC[:, 256 + s * 128 : 256 + (s + 1) * 128]], axis=0
        )
        BS[:, s, :] = x.T
    BR[me] = BS[me]
    peers(lambda d, t, l: send(BS.at[d], BR.at[me], bsem, t, l).start())
    lax.fori_loop(0, 8, send_e, 0)
    send_k(KFIRST, 64)

    def place(i, carry):
        o = lax.div(i, BANDS) * 16 + lax.rem(i, BANDS) + 4 * half
        t = jnp.concatenate([TT[k, pl.ds(o, 1), :] for k in range(2)], axis=1).astype(i32) - 1
        OHR[i] = jnp.where(iota((128, 256), 0) == (t & 127), 1.0, 0.0).astype(bf16)
        return carry

    lax.fori_loop(0, 8 * BANDS, place, 0)

    S3[...] = jnp.zeros((NB, 8, 128), f32)
    swap = jnp.where(
        iota((128, 128), 1) == (iota((128, 128), 0) & 63) * 2 + (iota((128, 128), 0) >> 6), 1.0, 0.0
    ).astype(bf16)
    weight = wgt_ref[...] * vld_ref[...].astype(f32)
    loads[3].wait()
    wait_n(BR, DEV - 1, bsem.at[1])
    parts = [split(BR[:, s, :]) for s in range(2)]
    for p in range(2):
        mine = dot(M[:, :DEV], parts[0][p], 1, 0) + dot(M[:, DEV:], parts[1][p], 1, 0)
        S3[:, p, :] = dot(mine.astype(bf16), swap, 1, 0)

    def predict(b, carry):
        PR[b] = dot(S3[b].astype(bf16), JAC[b], 1, 1)
        return carry

    lax.fori_loop(0, NB, predict, 0, unroll=8)
    resid = weight * (val_ref[...] - (PR[:, 0, :] + PR[:, 1, :]))
    for p, part in enumerate(split(resid)):
        S3[:, p, :] = part.astype(f32)

    def adjoin(b, carry):
        PR[b] = dot(S3[b].astype(bf16), JAC[b], 1, 0)
        return carry

    lax.fori_loop(0, NB, adjoin, 0, unroll=8)
    placed = jnp.zeros((128, 256), f32)
    for part in split(PR[:, 0, :] + PR[:, 1, :]):
        placed = placed + dot(dot(part, swap, 1, 1).astype(bf16), M, 0, 0)
    for s in range(2):
        for w in range(2):
            CS[:, s * 2 + w, :] = placed[w * 64 : (w + 1) * 64, s * 128 : (s + 1) * 128]
    CR[me] = CS[level]
    peers(lambda d, t, l: send(CS.at[lax.div(t, 2) * 16 + l], CR.at[me], csem, t, l).start())

    wait_home(KR, 64, ksem.at[1])
    wait_home(EN, 8, esem.at[1])
    halo_k = send(KR.at[pl.ds(32, 32)], KR.at[pl.ds(64 * half, 32)], fsem.at[0], mate, lat)
    halo_e = send(EN.at[pl.ds(4, 4)], EN.at[pl.ds(8 * half, 4)], fsem.at[1], mate, lat)
    halo_k.start()
    halo_e.start()
    halo_e.wait()
    for lb in range(BANDS):
        W[lb * 4 : lb * 4 + 4] = EN[lb].astype(f32).reshape(4, 16, 128)
    WT[0] = jnp.zeros((16, 128), f32)
    WT[49] = jnp.zeros((16, 128), f32)
    lane = iota((4, 8, 128), 2)
    halo_k.wait()

    def substeps(s):
        for step in range(2):
            for lb in range(BANDS):
                rows = slice(lb * 4, lb * 4 + 4)
                if step == 0:
                    k = KR[lb * 8 + s].astype(i32).astype(f32) * KSCALE + KMID
                    k = k.reshape(4, 16, 128)
                    KF[rows] = k
                else:
                    k = KF[rows]
                WT[1 + lb * 4 : 5 + lb * 4] = k * W[rows]
            for lb in range(BANDS):
                rows = slice(lb * 4, lb * 4 + 4)
                x = WT[1 + lb * 4 : 5 + lb * 4]
                even, odd = x[:, :8], x[:, 8:]
                a = pltpu.roll(odd, 1, axis=2)
                b = pltpu.roll(even, 127, axis=2)
                a = jnp.where(lane == 0, pltpu.roll(a, 1, axis=1), a)
                b = jnp.where(lane == 127, pltpu.roll(b, 7, axis=1), b)
                ends = WT[2 + lb * 4 : 6 + lb * 4] + WT[lb * 4 : lb * 4 + 4]
                w = W[rows]
                W[rows, :8] = w[:, :8] + (ends[:, :8] + (odd + a) - 4.0 * even)
                W[rows, 8:] = w[:, 8:] + (ends[:, 8:] + (even + b) - 4.0 * odd)

    def finish(s):
        for lb in range(BANDS):
            o = s * 16 + lb + 4 * half
            t = jnp.concatenate([TT[k, pl.ds(o, 1), :] for k in range(2)], axis=1).astype(i32) - 1
            mask = iota((32, 256), 0) == (t >> 7)
            terms = []
            for w in range(2):
                term = jnp.concatenate([RT[k * 2 + w, pl.ds(o, 1), :] for k in range(2)], axis=1)
                terms.append(split(term))
            lhs = jnp.concatenate(
                [jnp.where(mask, terms[w][p].astype(f32), 0.0) for p in range(2) for w in range(2)],
                axis=0,
            ).astype(bf16)
            y = dot(lhs, OHR[s * BANDS + lb], 1, 1)
            y = y[:64] + y[64:]
            rows = slice(lb * 4, lb * 4 + 4)
            for w in range(2):
                part = slice(w * 8, w * 8 + 8)
                W[rows, part] = W[rows, part] + y[w * 32 : w * 32 + 32].reshape(4, 8, 128)

        def deliver(j, carry):
            OS[s * 8 + j] = W[pl.ds(half * 16 + j * 4, 4)].reshape(CHUNK, 128).astype(bf16)
            to = half * 8 + j
            here = (s == tm) & (to == lat)

            @pl.when(here)
            def _():
                OR[level] = OS[s * 8 + j]

            @pl.when(jnp.logical_not(here))
            def _():
                send(OS.at[s * 8 + j], OR.at[level], osem, s, to).start()

            return carry

        lax.fori_loop(0, 8, deliver, 0)

    substeps(7)
    wait_n(CR, DEV - 1, csem.at[1])
    for q in range(4):
        RT[q] = CR[:, q, :].T

    def section(i, carry):
        s = 7 - i
        finish(s)
        W[...] = W[...].astype(bf16).astype(f32)
        substeps(s - 1)
        return carry

    lax.fori_loop(0, 7, section, 0)
    finish(0)

    wait_home(OR, 64, osem.at[1])

    def widen(l, carry):
        rows = pl.ds(pl.multiple_of(l * 64, 64), 64)
        k2[rows, :] = OR[l].astype(f32)
        return carry

    lax.fori_loop(0, 64, widen, 0, unroll=4)

    def store(r, carry):
        for g in range(8):
            x = jnp.concatenate(
                [k2[pl.ds(r * 16 + w * 8 + g, 64, stride=64), :] for w in range(2)], axis=1
            )
            out_ref[r, :, g * 256 : (g + 1) * 256] = dot(x.astype(bf16), apart, 1, 1)
        return carry

    lax.fori_loop(0, 4, store, 0)

    wait_n(AR, DEV - 1, asem.at[0])
    wait_n(BS, DEV - 1, bsem.at[0])
    wait_n(CR, DEV - 1, csem.at[0])
    wait_home(ES, 8, esem.at[0])
    wait_home(KS, 64, ksem.at[0])
    wait_home(OS, 64, osem.at[0])


def per_device(traj, kap, end, jac, val, wgt, vld, own, til):
    hbm = pl.BlockSpec(memory_space=pl.ANY)
    vmem = pl.BlockSpec(memory_space=pltpu.VMEM)
    dma = pltpu.SemaphoreType.DMA
    V = pltpu.VMEM
    out = pl.pallas_call(
        kernel,
        out_shape=jax.ShapeDtypeStruct((4, 64, 2048), f32),
        in_specs=[hbm] * 4 + [vmem] * 5,
        out_specs=vmem,
        scratch_shapes=[
            V((4, 64, 2048), f32), V((4, 64, 2048), f32), V((16, 256, 128), f32),
            V((4, 16, 2048), bf16), V((16, 64, 128), f32), V((NB, 128, 128), bf16),
            V((1, 2, 128), f32), V((DEV, 2, 128), f32), V((2, 128, 128), f32),
            V((256, 512), bf16), V((64, 512), f32), V((DEV, 2, 128), f32), V((DEV, 2, 128), f32),
            V((NB, 8, 128), f32), V((NB, 8, 128), f32), V((64, 4, 128), f32), V((DEV, 4, 128), f32),
            V((4, 128, 128), f32), V((8 * BANDS, 128, 256), bf16),
            V((64, CHUNK, 128), i16), V((8 * BANDS, CHUNK, 128), i16),
            V((8, CHUNK, 128), bf16), V((BANDS, CHUNK, 128), bf16),
            V((48, 16, 128), f32), V((50, 16, 128), f32), V((48, 16, 128), f32),
            V((64, CHUNK, 128), bf16), V((64, CHUNK, 128), bf16),
            dma((4,)), dma((2,)), dma((2,)), dma((2,)), dma((2,)), dma((2,)), dma((2, 2)), dma((2,)),
        ],
        compiler_params=pltpu.CompilerParams(
            has_side_effects=True, vmem_limit_bytes=56 << 20, collective_id=0
        ),
        name="adjoint_sweep",
    )(traj[0], kap[0], end, jac, val, wgt, vld, own.reshape(1, NB), til.reshape(1, NB))
    return out[None]


def solution(mesh):
    both = ("tm", "lat")
    in_specs = (
        P("tm", "lat", None, None),
        P("tm", "lat", None, None),
        P("lat", None, None),
        P(both, None, None),
        P(both, None),
        P(both, None),
        P(both, None),
        P(both, None),
        P(both),
    )
    return jax.shard_map(
        per_device, mesh=mesh, in_specs=in_specs, out_specs=P("tm", "lat", None, None),
        check_vma=False,
    )
```

```python
import jax
import jax.numpy as jnp
from jax import lax
from jax.experimental import pallas as pl
from jax.experimental.pallas import tpu as pltpu
from jax.sharding import PartitionSpec as P

f32, bf16, i16, i32 = jnp.float32, jnp.bfloat16, jnp.int16, jnp.int32
MESH = pl.DeviceIdType.MESH

DEV = 128
NB = 96
BANDS = 12
KFIRST = 32
CHUNK = 64
KMID, KSCALE = 0.13, 0.11 / 32700.0


def split(x):
    hi = x.astype(bf16)
    return hi, (x - hi.astype(f32)).astype(bf16)


def dot(a, b, ca, cb):
    return lax.dot_general(a, b, (((ca,), (cb,)), ((), ())), preferred_element_type=f32)


def iota(shape, dim):
    return lax.broadcasted_iota(i32, shape, dim)


def apart_matrix():
    target = (iota((256, 256), 1) & 127) * 2 + (iota((256, 256), 1) >> 7)
    return jnp.where(iota((256, 256), 0) == target, 1.0, 0.0).astype(bf16)


def kernel(
    traj_ref, kap_ref, end_ref, jac_ref, val_ref, wgt_ref, vld_ref, own_ref, til_ref,
    OR,
    TRJ, KIN, KQ, EIN, EQ, JAC,
    AS, AR, TT, LOH, ACC, BS, BR, S3, PR, CS, CR, RT, OHR,
    KS, KR, ES, EN, W, WT, KF, OS,
    lsem, asem, bsem, csem, ksem, esem, fsem, osem,
):
    tm = lax.axis_index("tm")
    lat = lax.axis_index("lat")
    me = tm * 16 + lat
    half = lax.rem(tm, 2)
    pair = lax.div(tm, 2)
    level = pair * 16 + lat
    mate = tm + 1 - 2 * half
    side = lax.div(lat, 8)
    home = side == half
    away = side != half

    def peers(fn):
        def step(i, carry):
            d = lax.rem(me + i, DEV)
            fn(d, lax.div(d, 16), lax.rem(d, 16))
            return carry

        lax.fori_loop(1, DEV, step, 0)

    def send(src, dst, sems, t, l):
        return pltpu.make_async_remote_copy(
            src, dst, sems.at[0], sems.at[1], device_id=(t, l), device_id_type=MESH
        )

    def wait_n(buf, n, sem):
        part = buf.at[pl.ds(0, n)]
        pltpu.make_async_copy(part, part, sem).wait()

    def wait_home(buf, n, sem):
        @pl.when(home)
        def _():
            wait_n(buf, n - 1, sem)

        @pl.when(away)
        def _():
            wait_n(buf, n, sem)

    loads = [
        pltpu.make_async_copy(kap_ref, KIN, lsem.at[0]),
        pltpu.make_async_copy(
            end_ref.at[:, pl.ds(pl.multiple_of(pair * 16, 16), 16), :], EIN, lsem.at[1]
        ),
        pltpu.make_async_copy(traj_ref, TRJ, lsem.at[2]),
        pltpu.make_async_copy(jac_ref, JAC, lsem.at[3]),
    ]
    for copy in loads:
        copy.start()
    barrier = pltpu.get_barrier_semaphore()
    peers(
        lambda d, t, l: pl.semaphore_signal(barrier, 1, device_id=(t, l), device_id_type=MESH)
    )

    eye = iota((NB, NB), 0) == iota((NB, NB), 1)
    own_row = own_ref[...].astype(f32)
    own = jnp.sum(jnp.where(eye, own_row, 0.0), axis=1, keepdims=True)
    til = jnp.sum(jnp.where(eye, til_ref[...].astype(f32), 0.0), axis=1, keepdims=True)
    same = (own == own_row) & (iota((NB, NB), 1) < iota((NB, NB), 0))
    rank = jnp.sum(jnp.where(same, 1.0, 0.0), axis=1, keepdims=True)
    hit = iota((NB, 2 * DEV), 1) == (rank * DEV + own).astype(i32)
    M = jnp.where(hit, 1.0, 0.0).astype(bf16)
    ids = jnp.sum(jnp.where(hit, til + 1.0, 0.0), axis=0, keepdims=True)
    AS[0, 0:1, :] = ids[:, :DEV]
    AS[0, 1:2, :] = ids[:, DEV:]
    AR[me] = AS[0]

    pl.semaphore_wait(barrier, DEV - 1)
    peers(lambda d, t, l: send(AS.at[0], AR.at[me], asem, t, l).start())

    apart = apart_matrix()

    loads[0].wait()

    def kap_row(r, carry):
        for g in range(8):
            q = jnp.round((KIN[r, :, g * 256 : (g + 1) * 256] - KMID) * (1.0 / KSCALE))
            a = jnp.round(q * (1.0 / 256.0))
            b = q - a * 256.0
            y = dot(jnp.concatenate([a, b], axis=0).astype(bf16), apart, 1, 0)
            y = y[:64] * 256.0 + y[64:]
            rows = pl.ds(pl.multiple_of(r * 64, 64), 64)
            KQ[g, rows, :] = y[:, :128]
            KQ[8 + g, rows, :] = y[:, 128:]
        return carry

    lax.fori_loop(0, 4, kap_row, 0)
    k2 = KQ.reshape(16 * 256, 128)

    def kap_level(l, carry):
        for r in range(4):
            q = k2[pl.ds(r * 64 + l, 16, stride=256), :]
            KS[l, r * 16 : (r + 1) * 16, :] = q.astype(i32).astype(i16)
        return carry

    lax.fori_loop(0, 64, kap_level, 0, unroll=2)

    lb_me = lat - 4 * side

    @pl.when(home)
    def _():
        KR[lb_me * 8 + tm] = KS[level]

    def send_k(lo, hi):
        def step(i, carry):
            l = lax.rem(level + i * 27, 64)

            @pl.when((i > 0) | away)
            def _():
                send(
                    KS.at[l], KR.at[lb_me * 8 + tm], ksem, lax.div(l, 16) * 2 + side, lax.rem(l, 16)
                ).start()

            return carry

        lax.fori_loop(lo, hi, step, 0)

    def send_e(i, carry):
        l = half * 8 + i

        @pl.when((l != lat) | away)
        def _():
            send(ES.at[i], EN.at[lb_me], esem, pair * 2 + side, l).start()

        return carry

    send_k(0, KFIRST)

    wait_n(AR, DEV - 1, asem.at[1])
    for s in range(2):
        TT[s] = AR[:, s, :].T
    tid = jnp.concatenate([TT[s, pl.ds(me, 1), :] for s in range(2)], axis=1).astype(i32) - 1
    low = (tid & 127) * 2
    group = jnp.concatenate([tid >> 7, tid >> 7], axis=1)
    LOH[...] = jnp.where(
        iota((256, 512), 0) == jnp.concatenate([low, low + 1], axis=1), 1.0, 0.0
    ).astype(bf16)
    ACC[...] = jnp.zeros((64, 512), f32)
    loads[2].wait()

    def gather_row(r, carry):
        total = ACC[...]
        for g in range(8):
            hi, lo = split(TRJ[r, :, g * 256 : (g + 1) * 256])
            y = dot(jnp.concatenate([hi, lo], axis=0), LOH[...], 1, 0)
            total = total + jnp.where(group == r * 8 + g, y[:64] + y[64:], 0.0)
        ACC[...] = total
        return carry

    lax.fori_loop(0, 4, gather_row, 0)
    for s in range(2):
        x = jnp.concatenate(
            [ACC[:, s * 128 : (s + 1) * 128], ACC[:, 256 + s * 128 : 256 + (s + 1) * 128]], axis=0
        )
        BS[:, s, :] = x.T
    BR[me] = BS[me]
    peers(lambda d, t, l: send(BS.at[d], BR.at[me], bsem, t, l).start())
    send_k(KFIRST, 64)

    loads[1].wait()
    for r in range(4):
        for g in range(8):
            y = dot(EIN[r, :, g * 256 : (g + 1) * 256], apart, 1, 0)
            EQ[g, r * 16 : (r + 1) * 16, :] = y[:, :128]
            EQ[8 + g, r * 16 : (r + 1) * 16, :] = y[:, 128:]
    e2 = EQ.reshape(16 * 64, 128)

    def end_level(l, carry):
        for r in range(4):
            rows = e2[pl.ds(r * 16 + half * 8 + l, 16, stride=64), :]
            ES[l, r * 16 : (r + 1) * 16, :] = rows.astype(bf16)
        return carry

    lax.fori_loop(0, 8, end_level, 0)

    @pl.when(home)
    def _():
        EN[lb_me] = ES[lat - 8 * half]

    lax.fori_loop(0, 8, send_e, 0)

    def place(i, carry):
        o = lax.div(i, BANDS) * 16 + lax.rem(i, BANDS) + 4 * half
        t = jnp.concatenate([TT[k, pl.ds(o, 1), :] for k in range(2)], axis=1).astype(i32) - 1
        OHR[i] = jnp.where(iota((128, 256), 0) == (t & 127), 1.0, 0.0).astype(bf16)
        return carry

    lax.fori_loop(0, 8 * BANDS, place, 0)

    S3[...] = jnp.zeros((NB, 8, 128), f32)
    swap = jnp.where(
        iota((128, 128), 1) == (iota((128, 128), 0) & 63) * 2 + (iota((128, 128), 0) >> 6), 1.0, 0.0
    ).astype(bf16)
    weight = wgt_ref[...] * vld_ref[...].astype(f32)
    loads[3].wait()
    wait_n(BR, DEV - 1, bsem.at[1])
    parts = [split(BR[:, s, :]) for s in range(2)]
    for p in range(2):
        mine = dot(M[:, :DEV], parts[0][p], 1, 0) + dot(M[:, DEV:], parts[1][p], 1, 0)
        S3[:, p, :] = dot(mine.astype(bf16), swap, 1, 0)

    def predict(b, carry):
        PR[b] = dot(S3[b].astype(bf16), JAC[b], 1, 1)
        return carry

    lax.fori_loop(0, NB, predict, 0, unroll=8)
    resid = weight * (val_ref[...] - (PR[:, 0, :] + PR[:, 1, :]))
    for p, part in enumerate(split(resid)):
        S3[:, p, :] = part.astype(f32)

    def adjoin(b, carry):
        PR[b] = dot(S3[b].astype(bf16), JAC[b], 1, 0)
        return carry

    lax.fori_loop(0, NB, adjoin, 0, unroll=8)
    placed = jnp.zeros((128, 256), f32)
    for part in split(PR[:, 0, :] + PR[:, 1, :]):
        placed = placed + dot(dot(part, swap, 1, 1).astype(bf16), M, 0, 0)
    for s in range(2):
        for w in range(2):
            CS[:, s * 2 + w, :] = placed[w * 64 : (w + 1) * 64, s * 128 : (s + 1) * 128]
    CR[me] = CS[level]
    peers(lambda d, t, l: send(CS.at[lax.div(t, 2) * 16 + l], CR.at[me], csem, t, l).start())

    wait_home(KR, 64, ksem.at[1])
    wait_home(EN, 8, esem.at[1])
    halo_k = send(KR.at[pl.ds(32, 32)], KR.at[pl.ds(64 * half, 32)], fsem.at[0], mate, lat)
    halo_e = send(EN.at[pl.ds(4, 4)], EN.at[pl.ds(8 * half, 4)], fsem.at[1], mate, lat)
    halo_k.start()
    halo_e.start()
    halo_e.wait()
    for lb in range(BANDS):
        W[lb * 4 : lb * 4 + 4] = EN[lb].astype(f32).reshape(4, 16, 128)
    WT[0] = jnp.zeros((16, 128), f32)
    WT[49] = jnp.zeros((16, 128), f32)
    lane = iota((4, 8, 128), 2)
    halo_k.wait()

    def substeps(s):
        for step in range(2):
            for lb in range(BANDS):
                rows = slice(lb * 4, lb * 4 + 4)
                if step == 0:
                    k = KR[lb * 8 + s].astype(i32).astype(f32) * KSCALE + KMID
                    k = k.reshape(4, 16, 128)
                    KF[rows] = k
                else:
                    k = KF[rows]
                WT[1 + lb * 4 : 5 + lb * 4] = k * W[rows]
            for lb in range(BANDS):
                rows = slice(lb * 4, lb * 4 + 4)
                x = WT[1 + lb * 4 : 5 + lb * 4]
                even, odd = x[:, :8], x[:, 8:]
                a = pltpu.roll(odd, 1, axis=2)
                b = pltpu.roll(even, 127, axis=2)
                a = jnp.where(lane == 0, pltpu.roll(a, 1, axis=1), a)
                b = jnp.where(lane == 127, pltpu.roll(b, 7, axis=1), b)
                ends = WT[2 + lb * 4 : 6 + lb * 4] + WT[lb * 4 : lb * 4 + 4]
                w = W[rows]
                W[rows, :8] = w[:, :8] + (ends[:, :8] + (odd + a) - 4.0 * even)
                W[rows, 8:] = w[:, 8:] + (ends[:, 8:] + (even + b) - 4.0 * odd)

    def finish(s):
        for lb in range(BANDS):
            o = s * 16 + lb + 4 * half
            t = jnp.concatenate([TT[k, pl.ds(o, 1), :] for k in range(2)], axis=1).astype(i32) - 1
            mask = iota((32, 256), 0) == (t >> 7)
            terms = []
            for w in range(2):
                term = jnp.concatenate([RT[k * 2 + w, pl.ds(o, 1), :] for k in range(2)], axis=1)
                terms.append(split(term))
            lhs = jnp.concatenate(
                [jnp.where(mask, terms[w][p].astype(f32), 0.0) for p in range(2) for w in range(2)],
                axis=0,
            ).astype(bf16)
            y = dot(lhs, OHR[s * BANDS + lb], 1, 1)
            y = y[:64] + y[64:]
            rows = slice(lb * 4, lb * 4 + 4)
            for w in range(2):
                part = slice(w * 8, w * 8 + 8)
                W[rows, part] = W[rows, part] + y[w * 32 : w * 32 + 32].reshape(4, 8, 128)

        def deliver(j, carry):
            j = lax.rem(j + lat + pair * 2, 8)
            OS[s * 8 + j] = W[pl.ds(half * 16 + j * 4, 4)].reshape(CHUNK, 128).astype(bf16)
            to = half * 8 + j
            here = (s == tm) & (to == lat)

            @pl.when(here)
            def _():
                OR[level] = OS[s * 8 + j]

            @pl.when(jnp.logical_not(here))
            def _():
                send(OS.at[s * 8 + j], OR.at[level], osem, s, to).start()

            return carry

        lax.fori_loop(0, 8, deliver, 0)

    substeps(7)
    wait_n(CR, DEV - 1, csem.at[1])
    for q in range(4):
        RT[q] = CR[:, q, :].T

    def section(i, carry):
        s = 7 - i
        finish(s)
        W[...] = W[...].astype(bf16).astype(f32)
        substeps(s - 1)
        return carry

    lax.fori_loop(0, 7, section, 0)
    finish(0)

    wait_home(OR, 64, osem.at[1])

    wait_n(AR, DEV - 1, asem.at[0])
    wait_n(BS, DEV - 1, bsem.at[0])
    wait_n(CR, DEV - 1, csem.at[0])
    wait_home(ES, 8, esem.at[0])
    wait_home(KS, 64, ksem.at[0])
    wait_home(OS, 64, osem.at[0])


def decode(or_ref, out_ref, wide, rows, sem):
    apart = apart_matrix()

    def widen(l, carry):
        wide[pl.ds(pl.multiple_of(l * 64, 64), 64), :] = or_ref[l].astype(f32)
        return carry

    lax.fori_loop(0, 64, widen, 0, unroll=4)

    def copy(r):
        return pltpu.make_async_copy(rows.at[r], out_ref.at[r], sem.at[r])

    for r in range(4):
        for g in range(8):
            x = jnp.concatenate(
                [wide[pl.ds(r * 16 + w * 8 + g, 64, stride=64), :] for w in range(2)], axis=1
            )
            rows[r, :, g * 256 : (g + 1) * 256] = dot(x.astype(bf16), apart, 1, 1)
        copy(r).start()
    for r in range(4):
        copy(r).wait()


def per_device(traj, kap, end, jac, val, wgt, vld, own, til):
    hbm = pl.BlockSpec(memory_space=pl.ANY)
    vmem = pl.BlockSpec(memory_space=pltpu.VMEM)
    dma = pltpu.SemaphoreType.DMA
    V = pltpu.VMEM
    out = pl.pallas_call(
        kernel,
        out_shape=jax.ShapeDtypeStruct((64, CHUNK, 128), bf16),
        in_specs=[hbm] * 4 + [vmem] * 5,
        out_specs=vmem,
        scratch_shapes=[
            V((4, 64, 2048), f32), V((4, 64, 2048), f32), V((16, 256, 128), f32),
            V((4, 16, 2048), bf16), V((16, 64, 128), f32), V((NB, 128, 128), bf16),
            V((1, 2, 128), f32), V((DEV, 2, 128), f32), V((2, 128, 128), f32),
            V((256, 512), bf16), V((64, 512), f32), V((DEV, 2, 128), f32), V((DEV, 2, 128), f32),
            V((NB, 8, 128), f32), V((NB, 8, 128), f32), V((64, 4, 128), f32), V((DEV, 4, 128), f32),
            V((4, 128, 128), f32), V((8 * BANDS, 128, 256), bf16),
            V((64, CHUNK, 128), i16), V((8 * BANDS, CHUNK, 128), i16),
            V((8, CHUNK, 128), bf16), V((BANDS, CHUNK, 128), bf16),
            V((48, 16, 128), f32), V((50, 16, 128), f32), V((48, 16, 128), f32),
            V((64, CHUNK, 128), bf16),
            dma((4,)), dma((2,)), dma((2,)), dma((2,)), dma((2,)), dma((2,)), dma((2, 2)), dma((2,)),
        ],
        compiler_params=pltpu.CompilerParams(
            has_side_effects=True, vmem_limit_bytes=56 << 20, collective_id=0
        ),
        name="adjoint_sweep",
    )(traj[0], kap[0], end, jac, val, wgt, vld, own.reshape(1, NB), til.reshape(1, NB))
    out = pl.pallas_call(
        decode,
        out_shape=jax.ShapeDtypeStruct((4, 64, 2048), f32),
        in_specs=[vmem],
        out_specs=hbm,
        scratch_shapes=[V((4096, 128), f32), V((4, 64, 2048), f32), dma((4,))],
        name="adjoint_decode",
    )(out)
    return out[None]


def solution(mesh):
    both = ("tm", "lat")
    in_specs = (
        P("tm", "lat", None, None),
        P("tm", "lat", None, None),
        P("lat", None, None),
        P(both, None, None),
        P(both, None),
        P(both, None),
        P(both, None),
        P(both, None),
        P(both),
    )
    return jax.shard_map(
        per_device, mesh=mesh, in_specs=in_specs, out_specs=P("tm", "lat", None, None),
        check_vma=False,
    )
```

```python
import jax
import jax.numpy as jnp
from jax import lax
from jax.experimental import pallas as pl
from jax.experimental.pallas import tpu as pltpu
from jax.sharding import PartitionSpec as P

f32, bf16, i16, i32 = jnp.float32, jnp.bfloat16, jnp.int16, jnp.int32
MESH = pl.DeviceIdType.MESH

DEV = 128
NB = 96
BANDS = 12
KFIRST, KNEXT = 8, 8
CHUNK = 64
KMID, KSCALE = 0.13, 0.11 / 32700.0


def split(x):
    hi = x.astype(bf16)
    return hi, (x - hi.astype(f32)).astype(bf16)


def dot(a, b, ca, cb):
    return lax.dot_general(a, b, (((ca,), (cb,)), ((), ())), preferred_element_type=f32)


def iota(shape, dim):
    return lax.broadcasted_iota(i32, shape, dim)


def apart_matrix():
    target = (iota((256, 256), 1) & 127) * 2 + (iota((256, 256), 1) >> 7)
    return jnp.where(iota((256, 256), 0) == target, 1.0, 0.0).astype(bf16)


def kernel(
    traj_ref, kap_ref, end_ref, jac_ref, val_ref, wgt_ref, vld_ref, own_ref, til_ref,
    OR,
    TRJ, KIN, KQ, EIN, EQ, JAC,
    AS, AR, TT, LOH, ACC, BS, BR, S3, PR, CS, CR, RT, OHR,
    KS, KR, ES, EN, W, WT, KF, OS,
    lsem, asem, bsem, csem, ksem, esem, fsem, osem,
):
    tm = lax.axis_index("tm")
    lat = lax.axis_index("lat")
    me = tm * 16 + lat
    half = lax.rem(tm, 2)
    pair = lax.div(tm, 2)
    level = pair * 16 + lat
    mate = tm + 1 - 2 * half
    side = lax.div(lat, 8)
    home = side == half
    away = side != half

    def peers(fn):
        def step(i, carry):
            d = lax.rem(me + i, DEV)
            fn(d, lax.div(d, 16), lax.rem(d, 16))
            return carry

        lax.fori_loop(1, DEV, step, 0, unroll=4)

    def send(src, dst, sems, t, l):
        return pltpu.make_async_remote_copy(
            src, dst, sems.at[0], sems.at[1], device_id=(t, l), device_id_type=MESH
        )

    def wait_n(buf, n, sem):
        part = buf.at[pl.ds(0, n)]
        pltpu.make_async_copy(part, part, sem).wait()

    def wait_home(buf, n, sem):
        @pl.when(home)
        def _():
            wait_n(buf, n - 1, sem)

        @pl.when(away)
        def _():
            wait_n(buf, n, sem)

    loads = [
        pltpu.make_async_copy(kap_ref, KIN, lsem.at[0]),
        pltpu.make_async_copy(
            end_ref.at[:, pl.ds(pl.multiple_of(pair * 16, 16), 16), :], EIN, lsem.at[1]
        ),
        pltpu.make_async_copy(traj_ref, TRJ, lsem.at[2]),
        pltpu.make_async_copy(jac_ref, JAC, lsem.at[3]),
    ]
    for copy in loads:
        copy.start()
    barrier = pltpu.get_barrier_semaphore()
    peers(
        lambda d, t, l: pl.semaphore_signal(barrier, 1, device_id=(t, l), device_id_type=MESH)
    )

    eye = iota((NB, NB), 0) == iota((NB, NB), 1)
    own_row = own_ref[...].astype(f32)
    own = jnp.sum(jnp.where(eye, own_row, 0.0), axis=1, keepdims=True)
    til = jnp.sum(jnp.where(eye, til_ref[...].astype(f32), 0.0), axis=1, keepdims=True)
    same = (own == own_row) & (iota((NB, NB), 1) < iota((NB, NB), 0))
    rank = jnp.sum(jnp.where(same, 1.0, 0.0), axis=1, keepdims=True)
    hit = iota((NB, 2 * DEV), 1) == (rank * DEV + own).astype(i32)
    M = jnp.where(hit, 1.0, 0.0).astype(bf16)
    ids = jnp.sum(jnp.where(hit, til + 1.0, 0.0), axis=0, keepdims=True)
    AS[0, 0:1, :] = ids[:, :DEV]
    AS[0, 1:2, :] = ids[:, DEV:]
    AR[me] = AS[0]

    pl.semaphore_wait(barrier, DEV - 1)
    peers(lambda d, t, l: send(AS.at[0], AR.at[me], asem, t, l).start())

    apart = apart_matrix()

    loads[0].wait()

    def kap_row(r, carry):
        for g in range(8):
            q = jnp.round((KIN[r, :, g * 256 : (g + 1) * 256] - KMID) * (1.0 / KSCALE))
            a = jnp.round(q * (1.0 / 256.0))
            b = q - a * 256.0
            y = dot(jnp.concatenate([a, b], axis=0).astype(bf16), apart, 1, 0)
            y = y[:64] * 256.0 + y[64:]
            rows = pl.ds(pl.multiple_of(r * 64, 64), 64)
            KQ[g, rows, :] = y[:, :128]
            KQ[8 + g, rows, :] = y[:, 128:]
        return carry

    lax.fori_loop(0, 4, kap_row, 0)
    k2 = KQ.reshape(16 * 256, 128)

    def kap_level(l, carry):
        for r in range(4):
            q = k2[pl.ds(r * 64 + l, 16, stride=256), :]
            KS[l, r * 16 : (r + 1) * 16, :] = q.astype(i32).astype(i16)
        return carry

    lax.fori_loop(0, 64, kap_level, 0, unroll=2)

    lb_me = lat - 4 * side

    @pl.when(home)
    def _():
        KR[lb_me * 8 + tm] = KS[level]

    def send_k(lo, hi):
        def step(i, carry):
            l = lax.rem(level + i * 27, 64)

            @pl.when((i > 0) | away)
            def _():
                send(
                    KS.at[l], KR.at[lb_me * 8 + tm], ksem, lax.div(l, 16) * 2 + side, lax.rem(l, 16)
                ).start()

            return carry

        lax.fori_loop(lo, hi, step, 0)

    def send_e(i, carry):
        l = half * 8 + i

        @pl.when((l != lat) | away)
        def _():
            send(ES.at[i], EN.at[lb_me], esem, pair * 2 + side, l).start()

        return carry

    send_k(0, KFIRST)

    wait_n(AR, DEV - 1, asem.at[1])
    send_k(KFIRST, KNEXT)
    for s in range(2):
        TT[s] = AR[:, s, :].T
    tid = jnp.concatenate([TT[s, pl.ds(me, 1), :] for s in range(2)], axis=1).astype(i32) - 1
    low = (tid & 127) * 2
    group = jnp.concatenate([tid >> 7, tid >> 7], axis=1)
    LOH[...] = jnp.where(
        iota((256, 512), 0) == jnp.concatenate([low, low + 1], axis=1), 1.0, 0.0
    ).astype(bf16)
    ACC[...] = jnp.zeros((64, 512), f32)
    loads[2].wait()

    def gather_row(r, carry):
        total = ACC[...]
        for g in range(8):
            hi, lo = split(TRJ[r, :, g * 256 : (g + 1) * 256])
            y = dot(jnp.concatenate([hi, lo], axis=0), LOH[...], 1, 0)
            total = total + jnp.where(group == r * 8 + g, y[:64] + y[64:], 0.0)
        ACC[...] = total
        return carry

    lax.fori_loop(0, 4, gather_row, 0)
    for s in range(2):
        x = jnp.concatenate(
            [ACC[:, s * 128 : (s + 1) * 128], ACC[:, 256 + s * 128 : 256 + (s + 1) * 128]], axis=0
        )
        BS[:, s, :] = x.T
    BR[me] = BS[me]
    peers(lambda d, t, l: send(BS.at[d], BR.at[me], bsem, t, l).start())
    send_k(KNEXT, 64)

    loads[1].wait()
    for r in range(4):
        for g in range(8):
            y = dot(EIN[r, :, g * 256 : (g + 1) * 256], apart, 1, 0)
            EQ[g, r * 16 : (r + 1) * 16, :] = y[:, :128]
            EQ[8 + g, r * 16 : (r + 1) * 16, :] = y[:, 128:]
    e2 = EQ.reshape(16 * 64, 128)

    def end_level(l, carry):
        for r in range(4):
            rows = e2[pl.ds(r * 16 + half * 8 + l, 16, stride=64), :]
            ES[l, r * 16 : (r + 1) * 16, :] = rows.astype(bf16)
        return carry

    lax.fori_loop(0, 8, end_level, 0)

    @pl.when(home)
    def _():
        EN[lb_me] = ES[lat - 8 * half]

    lax.fori_loop(0, 8, send_e, 0)

    def place(i, carry):
        o = lax.div(i, BANDS) * 16 + lax.rem(i, BANDS) + 4 * half
        t = jnp.concatenate([TT[k, pl.ds(o, 1), :] for k in range(2)], axis=1).astype(i32) - 1
        OHR[i] = jnp.where(iota((128, 256), 0) == (t & 127), 1.0, 0.0).astype(bf16)
        return carry

    lax.fori_loop(0, 8 * BANDS, place, 0)

    S3[...] = jnp.zeros((NB, 8, 128), f32)
    swap = jnp.where(
        iota((128, 128), 1) == (iota((128, 128), 0) & 63) * 2 + (iota((128, 128), 0) >> 6), 1.0, 0.0
    ).astype(bf16)
    weight = wgt_ref[...] * vld_ref[...].astype(f32)
    loads[3].wait()
    wait_n(BR, DEV - 1, bsem.at[1])
    parts = [split(BR[:, s, :]) for s in range(2)]
    for p in range(2):
        mine = dot(M[:, :DEV], parts[0][p], 1, 0) + dot(M[:, DEV:], parts[1][p], 1, 0)
        S3[:, p, :] = dot(mine.astype(bf16), swap, 1, 0)

    def predict(b, carry):
        PR[b] = dot(S3[b].astype(bf16), JAC[b], 1, 1)
        return carry

    lax.fori_loop(0, NB, predict, 0, unroll=8)
    resid = weight * (val_ref[...] - (PR[:, 0, :] + PR[:, 1, :]))
    for p, part in enumerate(split(resid)):
        S3[:, p, :] = part.astype(f32)

    def adjoin(b, carry):
        PR[b] = dot(S3[b].astype(bf16), JAC[b], 1, 0)
        return carry

    lax.fori_loop(0, NB, adjoin, 0, unroll=8)
    placed = jnp.zeros((128, 256), f32)
    for part in split(PR[:, 0, :] + PR[:, 1, :]):
        placed = placed + dot(dot(part, swap, 1, 1).astype(bf16), M, 0, 0)
    for s in range(2):
        for w in range(2):
            CS[:, s * 2 + w, :] = placed[w * 64 : (w + 1) * 64, s * 128 : (s + 1) * 128]
    CR[me] = CS[level]
    peers(lambda d, t, l: send(CS.at[lax.div(t, 2) * 16 + l], CR.at[me], csem, t, l).start())

    wait_home(KR, 64, ksem.at[1])
    wait_home(EN, 8, esem.at[1])
    halo_k = send(KR.at[pl.ds(32, 32)], KR.at[pl.ds(64 * half, 32)], fsem.at[0], mate, lat)
    halo_e = send(EN.at[pl.ds(4, 4)], EN.at[pl.ds(8 * half, 4)], fsem.at[1], mate, lat)
    halo_k.start()
    halo_e.start()
    halo_e.wait()
    for lb in range(BANDS):
        W[lb * 4 : lb * 4 + 4] = EN[lb].astype(f32).reshape(4, 16, 128)
    WT[0] = jnp.zeros((16, 128), f32)
    WT[49] = jnp.zeros((16, 128), f32)
    lane = iota((4, 8, 128), 2)
    halo_k.wait()

    def substeps(s):
        for step in range(2):
            for lb in range(BANDS):
                rows = slice(lb * 4, lb * 4 + 4)
                if step == 0:
                    k = KR[lb * 8 + s].astype(i32).astype(f32) * KSCALE + KMID
                    k = k.reshape(4, 16, 128)
                    KF[rows] = k
                else:
                    k = KF[rows]
                WT[1 + lb * 4 : 5 + lb * 4] = k * W[rows]
            for lb in range(BANDS):
                rows = slice(lb * 4, lb * 4 + 4)
                x = WT[1 + lb * 4 : 5 + lb * 4]
                even, odd = x[:, :8], x[:, 8:]
                a = pltpu.roll(odd, 1, axis=2)
                b = pltpu.roll(even, 127, axis=2)
                a = jnp.where(lane == 0, pltpu.roll(a, 1, axis=1), a)
                b = jnp.where(lane == 127, pltpu.roll(b, 7, axis=1), b)
                ends = WT[2 + lb * 4 : 6 + lb * 4] + WT[lb * 4 : lb * 4 + 4]
                w = W[rows]
                W[rows, :8] = w[:, :8] + (ends[:, :8] + (odd + a) - 4.0 * even)
                W[rows, 8:] = w[:, 8:] + (ends[:, 8:] + (even + b) - 4.0 * odd)

    def finish(s):
        for lb in range(BANDS):
            o = s * 16 + lb + 4 * half
            t = jnp.concatenate([TT[k, pl.ds(o, 1), :] for k in range(2)], axis=1).astype(i32) - 1
            mask = iota((32, 256), 0) == (t >> 7)
            terms = []
            for w in range(2):
                term = jnp.concatenate([RT[k * 2 + w, pl.ds(o, 1), :] for k in range(2)], axis=1)
                terms.append(split(term))
            lhs = jnp.concatenate(
                [jnp.where(mask, terms[w][p].astype(f32), 0.0) for p in range(2) for w in range(2)],
                axis=0,
            ).astype(bf16)
            y = dot(lhs, OHR[s * BANDS + lb], 1, 1)
            y = y[:64] + y[64:]
            rows = slice(lb * 4, lb * 4 + 4)
            for w in range(2):
                part = slice(w * 8, w * 8 + 8)
                W[rows, part] = W[rows, part] + y[w * 32 : w * 32 + 32].reshape(4, 8, 128)

        for j in range(8):
            rows = W[pl.ds(half * 16 + j * 4, 4)]
            OS[s * 8 + j] = rows.reshape(CHUNK, 128).astype(bf16)

    def deliver(s, j):
        here = (s == tm) & (half * 8 + j == lat)

        @pl.when(jnp.logical_not(here))
        def _():
            send(OS.at[s * 8 + j], OR.at[level], osem, s, half * 8 + j).start()

    def deliver_early(s):
        def step(i, carry):
            deliver(s, lax.rem(i + lat + pair * 2, 8))
            return carry

        lax.fori_loop(0, 8, step, 0)

    def deliver_late(i, carry):
        q = lax.rem(i, 5)
        s = jnp.int32(0)
        for k, v in enumerate([0, 2, 4, 6, 1]):
            s = jnp.where(q == k, v, s)
        deliver(s, lax.rem(lax.div(i, 5) + lat + pair * 2 + q, 8))
        return carry

    substeps(7)
    wait_n(CR, DEV - 1, csem.at[1])
    for q in range(4):
        RT[q] = CR[:, q, :].T

    def section(i, carry):
        s = 7 - i
        finish(s)

        @pl.when((s == 7) | (s == 5) | (s == 3))
        def _():
            deliver_early(s)

        W[...] = W[...].astype(bf16).astype(f32)
        substeps(s - 1)
        return carry

    lax.fori_loop(0, 7, section, 0)
    finish(0)
    lax.fori_loop(0, 40, deliver_late, 0)

    @pl.when(home)
    def _():
        OR[level] = OS[tm * 8 + lat - half * 8]

    wait_home(OR, 64, osem.at[1])

    wait_n(AR, DEV - 1, asem.at[0])
    wait_n(BS, DEV - 1, bsem.at[0])
    wait_n(CR, DEV - 1, csem.at[0])
    wait_home(ES, 8, esem.at[0])
    wait_home(KS, 64, ksem.at[0])
    wait_home(OS, 64, osem.at[0])


def decode(or_ref, out_ref, wide, rows, sem):
    apart = apart_matrix()

    def widen(l, carry):
        wide[pl.ds(pl.multiple_of(l * 64, 64), 64), :] = or_ref[l].astype(f32)
        return carry

    lax.fori_loop(0, 64, widen, 0, unroll=4)

    def copy(r):
        return pltpu.make_async_copy(rows.at[r], out_ref.at[r], sem.at[r])

    for r in range(4):
        for g in range(8):
            x = jnp.concatenate(
                [wide[pl.ds(r * 16 + w * 8 + g, 64, stride=64), :] for w in range(2)], axis=1
            )
            rows[r, :, g * 256 : (g + 1) * 256] = dot(x.astype(bf16), apart, 1, 1)
        copy(r).start()
    for r in range(4):
        copy(r).wait()


def per_device(traj, kap, end, jac, val, wgt, vld, own, til):
    hbm = pl.BlockSpec(memory_space=pl.ANY)
    vmem = pl.BlockSpec(memory_space=pltpu.VMEM)
    dma = pltpu.SemaphoreType.DMA
    V = pltpu.VMEM
    out = pl.pallas_call(
        kernel,
        out_shape=jax.ShapeDtypeStruct((64, CHUNK, 128), bf16),
        in_specs=[hbm] * 4 + [vmem] * 5,
        out_specs=vmem,
        scratch_shapes=[
            V((4, 64, 2048), f32), V((4, 64, 2048), f32), V((16, 256, 128), f32),
            V((4, 16, 2048), bf16), V((16, 64, 128), f32), V((NB, 128, 128), bf16),
            V((1, 2, 128), f32), V((DEV, 2, 128), f32), V((2, 128, 128), f32),
            V((256, 512), bf16), V((64, 512), f32), V((DEV, 2, 128), f32), V((DEV, 2, 128), f32),
            V((NB, 8, 128), f32), V((NB, 8, 128), f32), V((64, 4, 128), f32), V((DEV, 4, 128), f32),
            V((4, 128, 128), f32), V((8 * BANDS, 128, 256), bf16),
            V((64, CHUNK, 128), i16), V((8 * BANDS, CHUNK, 128), i16),
            V((8, CHUNK, 128), bf16), V((BANDS, CHUNK, 128), bf16),
            V((48, 16, 128), f32), V((50, 16, 128), f32), V((48, 16, 128), f32),
            V((64, CHUNK, 128), bf16),
            dma((4,)), dma((2,)), dma((2,)), dma((2,)), dma((2,)), dma((2,)), dma((2, 2)), dma((2,)),
        ],
        compiler_params=pltpu.CompilerParams(
            has_side_effects=True, vmem_limit_bytes=56 << 20, collective_id=0
        ),
        name="adjoint_sweep",
    )(traj[0], kap[0], end, jac, val, wgt, vld, own.reshape(1, NB), til.reshape(1, NB))
    out = pl.pallas_call(
        decode,
        out_shape=jax.ShapeDtypeStruct((4, 64, 2048), f32),
        in_specs=[vmem],
        out_specs=hbm,
        scratch_shapes=[V((4096, 128), f32), V((4, 64, 2048), f32), dma((4,))],
        name="adjoint_decode",
    )(out)
    return out[None]


def solution(mesh):
    both = ("tm", "lat")
    in_specs = (
        P("tm", "lat", None, None),
        P("tm", "lat", None, None),
        P("lat", None, None),
        P(both, None, None),
        P(both, None),
        P(both, None),
        P(both, None),
        P(both, None),
        P(both),
    )
    return jax.shard_map(
        per_device, mesh=mesh, in_specs=in_specs, out_specs=P("tm", "lat", None, None),
        check_vma=False,
    )
```

```python
import jax
import jax.numpy as jnp
from jax import lax
from jax.experimental import pallas as pl
from jax.experimental.pallas import tpu as pltpu
from jax.sharding import PartitionSpec as P

f32, bf16, i16, i32 = jnp.float32, jnp.bfloat16, jnp.int16, jnp.int32
MESH = pl.DeviceIdType.MESH

DEV = 128
NB = 96
BANDS = 12
KFIRST = 8
CHUNK = 64
KMID, KSCALE = 0.13, 0.11 / 32700.0


def split(x):
    hi = x.astype(bf16)
    return hi, (x - hi.astype(f32)).astype(bf16)


def dot(a, b, ca, cb):
    return lax.dot_general(a, b, (((ca,), (cb,)), ((), ())), preferred_element_type=f32)


def iota(shape, dim):
    return lax.broadcasted_iota(i32, shape, dim)


def apart_matrix():
    target = (iota((256, 256), 1) & 127) * 2 + (iota((256, 256), 1) >> 7)
    return jnp.where(iota((256, 256), 0) == target, 1.0, 0.0).astype(bf16)


def kernel(
    traj_ref, kap_ref, end_ref, jac_ref, val_ref, wgt_ref, vld_ref, own_ref, til_ref,
    OR,
    TRJ, KIN, KQ, EIN, EQ, JAC,
    AS, AR, TT, LOH, ACC, BS, BR, S3, PR, CS, CR, RT, OHR,
    KS, KR, ES, EN, W, WT, KF, OS,
    lsem, asem, bsem, csem, ksem, esem, fsem, osem,
):
    tm = lax.axis_index("tm")
    lat = lax.axis_index("lat")
    me = tm * 16 + lat
    half = lax.rem(tm, 2)
    pair = lax.div(tm, 2)
    level = pair * 16 + lat
    mate = tm + 1 - 2 * half
    side = lax.div(lat, 8)
    home = side == half
    away = side != half

    def peers(fn):
        def step(i, carry):
            d = lax.rem(me + i, DEV)
            fn(d, lax.div(d, 16), lax.rem(d, 16))
            return carry

        lax.fori_loop(1, DEV, step, 0, unroll=4)

    def send(src, dst, sems, t, l):
        return pltpu.make_async_remote_copy(
            src, dst, sems.at[0], sems.at[1], device_id=(t, l), device_id_type=MESH
        )

    def wait_n(buf, n, sem):
        part = buf.at[pl.ds(0, n)]
        pltpu.make_async_copy(part, part, sem).wait()

    def wait_home(buf, n, sem):
        @pl.when(home)
        def _():
            wait_n(buf, n - 1, sem)

        @pl.when(away)
        def _():
            wait_n(buf, n, sem)

    loads = [
        pltpu.make_async_copy(kap_ref, KIN, lsem.at[0]),
        pltpu.make_async_copy(
            end_ref.at[:, pl.ds(pl.multiple_of(pair * 16, 16), 16), :], EIN, lsem.at[1]
        ),
        pltpu.make_async_copy(traj_ref, TRJ, lsem.at[2]),
        pltpu.make_async_copy(jac_ref, JAC, lsem.at[3]),
    ]
    for copy in loads:
        copy.start()
    barrier = pltpu.get_barrier_semaphore()
    peers(
        lambda d, t, l: pl.semaphore_signal(barrier, 1, device_id=(t, l), device_id_type=MESH)
    )

    eye = iota((NB, NB), 0) == iota((NB, NB), 1)
    own_row = own_ref[...].astype(f32)
    own = jnp.sum(jnp.where(eye, own_row, 0.0), axis=1, keepdims=True)
    til = jnp.sum(jnp.where(eye, til_ref[...].astype(f32), 0.0), axis=1, keepdims=True)
    same = (own == own_row) & (iota((NB, NB), 1) < iota((NB, NB), 0))
    rank = jnp.sum(jnp.where(same, 1.0, 0.0), axis=1, keepdims=True)
    hit = iota((NB, 2 * DEV), 1) == (rank * DEV + own).astype(i32)
    M = jnp.where(hit, 1.0, 0.0).astype(bf16)
    ids = jnp.sum(jnp.where(hit, til + 1.0, 0.0), axis=0, keepdims=True)
    AS[0, 0:1, :] = ids[:, :DEV]
    AS[0, 1:2, :] = ids[:, DEV:]
    AR[me] = AS[0]

    pl.semaphore_wait(barrier, DEV - 1)
    peers(lambda d, t, l: send(AS.at[0], AR.at[me], asem, t, l).start())

    apart = apart_matrix()

    loads[0].wait()

    def kap_row(r, carry):
        for g in range(8):
            q = jnp.round((KIN[r, :, g * 256 : (g + 1) * 256] - KMID) * (1.0 / KSCALE))
            a = jnp.round(q * (1.0 / 256.0))
            b = q - a * 256.0
            y = dot(jnp.concatenate([a, b], axis=0).astype(bf16), apart, 1, 0)
            y = y[:64] * 256.0 + y[64:]
            rows = pl.ds(pl.multiple_of(r * 64, 64), 64)
            KQ[g, rows, :] = y[:, :128]
            KQ[8 + g, rows, :] = y[:, 128:]
        return carry

    lax.fori_loop(0, 4, kap_row, 0)
    k2 = KQ.reshape(16 * 256, 128)

    def kap_level(l, carry):
        for r in range(4):
            q = k2[pl.ds(r * 64 + l, 16, stride=256), :]
            KS[l, r * 16 : (r + 1) * 16, :] = q.astype(i32).astype(i16)
        return carry

    lax.fori_loop(0, 64, kap_level, 0, unroll=2)

    lb_me = lat - 4 * side

    @pl.when(home)
    def _():
        KR[lb_me * 8 + tm] = KS[level]

    def send_k(lo, hi):
        def step(i, carry):
            l = lax.rem(level + i * 27, 64)

            @pl.when((i > 0) | away)
            def _():
                send(
                    KS.at[l], KR.at[lb_me * 8 + tm], ksem, lax.div(l, 16) * 2 + side, lax.rem(l, 16)
                ).start()

            return carry

        lax.fori_loop(lo, hi, step, 0)

    def send_e(i, carry):
        i = lax.rem(i + lat, 8)
        l = half * 8 + i

        @pl.when((l != lat) | away)
        def _():
            send(ES.at[i], EN.at[lb_me], esem, pair * 2 + side, l).start()

        return carry

    send_k(0, KFIRST)

    loads[1].wait()
    for r in range(4):
        for g in range(8):
            y = dot(EIN[r, :, g * 256 : (g + 1) * 256], apart, 1, 0)
            EQ[g, r * 16 : (r + 1) * 16, :] = y[:, :128]
            EQ[8 + g, r * 16 : (r + 1) * 16, :] = y[:, 128:]
    e2 = EQ.reshape(16 * 64, 128)

    def end_level(l, carry):
        for r in range(4):
            rows = e2[pl.ds(r * 16 + half * 8 + l, 16, stride=64), :]
            ES[l, r * 16 : (r + 1) * 16, :] = rows.astype(bf16)
        return carry

    lax.fori_loop(0, 8, end_level, 0)

    @pl.when(home)
    def _():
        EN[lb_me] = ES[lat - 8 * half]

    lax.fori_loop(0, 8, send_e, 0)
    S3[...] = jnp.zeros((NB, 8, 128), f32)

    wait_n(AR, DEV - 1, asem.at[1])
    for s in range(2):
        TT[s] = AR[:, s, :].T
    tid = jnp.concatenate([TT[s, pl.ds(me, 1), :] for s in range(2)], axis=1).astype(i32) - 1
    low = (tid & 127) * 2
    group = jnp.concatenate([tid >> 7, tid >> 7], axis=1)
    LOH[...] = jnp.where(
        iota((256, 512), 0) == jnp.concatenate([low, low + 1], axis=1), 1.0, 0.0
    ).astype(bf16)
    ACC[...] = jnp.zeros((64, 512), f32)
    loads[2].wait()

    def gather_row(r, carry):
        total = ACC[...]
        for g in range(8):
            hi, lo = split(TRJ[r, :, g * 256 : (g + 1) * 256])
            y = dot(jnp.concatenate([hi, lo], axis=0), LOH[...], 1, 0)
            total = total + jnp.where(group == r * 8 + g, y[:64] + y[64:], 0.0)
        ACC[...] = total
        return carry

    lax.fori_loop(0, 4, gather_row, 0)
    for s in range(2):
        x = jnp.concatenate(
            [ACC[:, s * 128 : (s + 1) * 128], ACC[:, 256 + s * 128 : 256 + (s + 1) * 128]], axis=0
        )
        BS[:, s, :] = x.T
    BR[me] = BS[me]
    peers(lambda d, t, l: send(BS.at[d], BR.at[me], bsem, t, l).start())
    send_k(KFIRST, 64)


    def place(i, carry):
        o = lax.div(i, BANDS) * 16 + lax.rem(i, BANDS) + 4 * half
        t = jnp.concatenate([TT[k, pl.ds(o, 1), :] for k in range(2)], axis=1).astype(i32) - 1
        OHR[i] = jnp.where(iota((128, 256), 0) == (t & 127), 1.0, 0.0).astype(bf16)
        return carry

    lax.fori_loop(0, 8 * BANDS, place, 0)

    swap = jnp.where(
        iota((128, 128), 1) == (iota((128, 128), 0) & 63) * 2 + (iota((128, 128), 0) >> 6), 1.0, 0.0
    ).astype(bf16)
    weight = wgt_ref[...] * vld_ref[...].astype(f32)
    loads[3].wait()
    wait_n(BR, DEV - 1, bsem.at[1])
    parts = [split(BR[:, s, :]) for s in range(2)]
    for p in range(2):
        mine = dot(M[:, :DEV], parts[0][p], 1, 0) + dot(M[:, DEV:], parts[1][p], 1, 0)
        S3[:, p, :] = dot(mine.astype(bf16), swap, 1, 0)

    def predict(b, carry):
        PR[b] = dot(S3[b].astype(bf16), JAC[b], 1, 1)
        return carry

    lax.fori_loop(0, NB, predict, 0, unroll=32)
    resid = weight * (val_ref[...] - (PR[:, 0, :] + PR[:, 1, :]))
    for p, part in enumerate(split(resid)):
        S3[:, p, :] = part.astype(f32)

    def adjoin(b, carry):
        PR[b] = dot(S3[b].astype(bf16), JAC[b], 1, 0)
        return carry

    lax.fori_loop(0, NB, adjoin, 0, unroll=32)
    placed = jnp.zeros((128, 256), f32)
    for part in split(PR[:, 0, :] + PR[:, 1, :]):
        placed = placed + dot(dot(part, swap, 1, 1).astype(bf16), M, 0, 0)
    for s in range(2):
        for w in range(2):
            CS[:, s * 2 + w, :] = placed[w * 64 : (w + 1) * 64, s * 128 : (s + 1) * 128]
    CR[me] = CS[level]
    peers(lambda d, t, l: send(CS.at[lax.div(t, 2) * 16 + l], CR.at[me], csem, t, l).start())

    wait_home(KR, 64, ksem.at[1])
    wait_home(EN, 8, esem.at[1])
    halo_k = send(KR.at[pl.ds(32, 32)], KR.at[pl.ds(64 * half, 32)], fsem.at[0], mate, lat)
    halo_e = send(EN.at[pl.ds(4, 4)], EN.at[pl.ds(8 * half, 4)], fsem.at[1], mate, lat)
    halo_k.start()
    halo_e.start()
    halo_e.wait()
    for lb in range(BANDS):
        W[lb * 4 : lb * 4 + 4] = EN[lb].astype(f32).reshape(4, 16, 128)
    WT[0] = jnp.zeros((16, 128), f32)
    WT[49] = jnp.zeros((16, 128), f32)
    lane = iota((4, 8, 128), 2)
    halo_k.wait()

    def substeps(s):
        for step in range(2):
            for lb in range(BANDS):
                rows = slice(lb * 4, lb * 4 + 4)
                if step == 0:
                    k = KR[lb * 8 + s].astype(i32).astype(f32) * KSCALE + KMID
                    k = k.reshape(4, 16, 128)
                    KF[rows] = k
                else:
                    k = KF[rows]
                WT[1 + lb * 4 : 5 + lb * 4] = k * W[rows]
            for lb in range(BANDS):
                rows = slice(lb * 4, lb * 4 + 4)
                x = WT[1 + lb * 4 : 5 + lb * 4]
                even, odd = x[:, :8], x[:, 8:]
                a = pltpu.roll(odd, 1, axis=2)
                b = pltpu.roll(even, 127, axis=2)
                a = jnp.where(lane == 0, pltpu.roll(a, 1, axis=1), a)
                b = jnp.where(lane == 127, pltpu.roll(b, 7, axis=1), b)
                ends = WT[2 + lb * 4 : 6 + lb * 4] + WT[lb * 4 : lb * 4 + 4]
                w = W[rows]
                W[rows, :8] = w[:, :8] + (ends[:, :8] + (odd + a) - 4.0 * even)
                W[rows, 8:] = w[:, 8:] + (ends[:, 8:] + (even + b) - 4.0 * odd)

    def finish(s):
        for lb in range(BANDS):
            o = s * 16 + lb + 4 * half
            t = jnp.concatenate([TT[k, pl.ds(o, 1), :] for k in range(2)], axis=1).astype(i32) - 1
            mask = iota((32, 256), 0) == (t >> 7)
            terms = []
            for w in range(2):
                term = jnp.concatenate([RT[k * 2 + w, pl.ds(o, 1), :] for k in range(2)], axis=1)
                terms.append(split(term))
            lhs = jnp.concatenate(
                [jnp.where(mask, terms[w][p].astype(f32), 0.0) for p in range(2) for w in range(2)],
                axis=0,
            ).astype(bf16)
            y = dot(lhs, OHR[s * BANDS + lb], 1, 1)
            y = y[:64] + y[64:]
            rows = slice(lb * 4, lb * 4 + 4)
            for w in range(2):
                part = slice(w * 8, w * 8 + 8)
                W[rows, part] = W[rows, part] + y[w * 32 : w * 32 + 32].reshape(4, 8, 128)

        for j in range(8):
            rows = W[pl.ds(half * 16 + j * 4, 4)]
            OS[s * 8 + j] = rows.reshape(CHUNK, 128).astype(bf16)

    def deliver(s, j):
        here = (s == tm) & (half * 8 + j == lat)

        @pl.when(jnp.logical_not(here))
        def _():
            send(OS.at[s * 8 + j], OR.at[level], osem, s, half * 8 + j).start()

    def deliver_early(s):
        def step(i, carry):
            deliver(s, lax.rem(i + lat + pair * 2, 8))
            return carry

        lax.fori_loop(0, 8, step, 0)

    def deliver_late(i, carry):
        q = lax.rem(i, 5)
        s = jnp.int32(0)
        for k, v in enumerate([0, 2, 4, 6, 1]):
            s = jnp.where(q == k, v, s)
        deliver(s, lax.rem(lax.div(i, 5) + lat + pair * 2 + q, 8))
        return carry

    substeps(7)
    wait_n(CR, DEV - 1, csem.at[1])
    for q in range(4):
        RT[q] = CR[:, q, :].T

    def section(i, carry):
        s = 7 - i
        finish(s)

        @pl.when((s == 7) | (s == 5) | (s == 3))
        def _():
            deliver_early(s)

        W[...] = W[...].astype(bf16).astype(f32)
        substeps(s - 1)
        return carry

    lax.fori_loop(0, 7, section, 0)
    finish(0)
    lax.fori_loop(0, 40, deliver_late, 0)

    @pl.when(home)
    def _():
        OR[level] = OS[tm * 8 + lat - half * 8]

    wait_home(OR, 64, osem.at[1])

    wait_n(AR, DEV - 1, asem.at[0])
    wait_n(BS, DEV - 1, bsem.at[0])
    wait_n(CR, DEV - 1, csem.at[0])
    wait_home(ES, 8, esem.at[0])
    wait_home(KS, 64, ksem.at[0])
    wait_home(OS, 64, osem.at[0])


def decode(or_ref, out_ref, wide, rows, sem):
    apart = apart_matrix()

    def widen(l, carry):
        wide[pl.ds(pl.multiple_of(l * 64, 64), 64), :] = or_ref[l].astype(f32)
        return carry

    lax.fori_loop(0, 64, widen, 0, unroll=4)

    def copy(r):
        return pltpu.make_async_copy(rows.at[r], out_ref.at[r], sem.at[r])

    for r in range(4):
        for g in range(8):
            x = jnp.concatenate(
                [wide[pl.ds(r * 16 + w * 8 + g, 64, stride=64), :] for w in range(2)], axis=1
            )
            rows[r, :, g * 256 : (g + 1) * 256] = dot(x.astype(bf16), apart, 1, 1)
        copy(r).start()
    for r in range(4):
        copy(r).wait()


def per_device(traj, kap, end, jac, val, wgt, vld, own, til):
    hbm = pl.BlockSpec(memory_space=pl.ANY)
    vmem = pl.BlockSpec(memory_space=pltpu.VMEM)
    dma = pltpu.SemaphoreType.DMA
    V = pltpu.VMEM
    out = pl.pallas_call(
        kernel,
        out_shape=jax.ShapeDtypeStruct((64, CHUNK, 128), bf16),
        in_specs=[hbm] * 4 + [vmem] * 5,
        out_specs=vmem,
        scratch_shapes=[
            V((4, 64, 2048), f32), V((4, 64, 2048), f32), V((16, 256, 128), f32),
            V((4, 16, 2048), bf16), V((16, 64, 128), f32), V((NB, 128, 128), bf16),
            V((1, 2, 128), f32), V((DEV, 2, 128), f32), V((2, 128, 128), f32),
            V((256, 512), bf16), V((64, 512), f32), V((DEV, 2, 128), f32), V((DEV, 2, 128), f32),
            V((NB, 8, 128), f32), V((NB, 8, 128), f32), V((64, 4, 128), f32), V((DEV, 4, 128), f32),
            V((4, 128, 128), f32), V((8 * BANDS, 128, 256), bf16),
            V((64, CHUNK, 128), i16), V((8 * BANDS, CHUNK, 128), i16),
            V((8, CHUNK, 128), bf16), V((BANDS, CHUNK, 128), bf16),
            V((48, 16, 128), f32), V((50, 16, 128), f32), V((48, 16, 128), f32),
            V((64, CHUNK, 128), bf16),
            dma((4,)), dma((2,)), dma((2,)), dma((2,)), dma((2,)), dma((2,)), dma((2, 2)), dma((2,)),
        ],
        compiler_params=pltpu.CompilerParams(
            has_side_effects=True, vmem_limit_bytes=56 << 20, collective_id=0
        ),
        name="adjoint_sweep",
    )(traj[0], kap[0], end, jac, val, wgt, vld, own.reshape(1, NB), til.reshape(1, NB))
    out = pl.pallas_call(
        decode,
        out_shape=jax.ShapeDtypeStruct((4, 64, 2048), f32),
        in_specs=[vmem],
        out_specs=hbm,
        scratch_shapes=[V((4096, 128), f32), V((4, 64, 2048), f32), dma((4,))],
        name="adjoint_decode",
    )(out)
    return out[None]


def solution(mesh):
    both = ("tm", "lat")
    in_specs = (
        P("tm", "lat", None, None),
        P("tm", "lat", None, None),
        P("lat", None, None),
        P(both, None, None),
        P(both, None),
        P(both, None),
        P(both, None),
        P(both, None),
        P(both),
    )
    return jax.shard_map(
        per_device, mesh=mesh, in_specs=in_specs, out_specs=P("tm", "lat", None, None),
        check_vma=False,
    )
```

```python
import jax
import jax.numpy as jnp
from jax import lax
from jax.experimental import pallas as pl
from jax.experimental.pallas import tpu as pltpu
from jax.sharding import PartitionSpec as P

f32, bf16, i16, i32 = jnp.float32, jnp.bfloat16, jnp.int16, jnp.int32
MESH = pl.DeviceIdType.MESH

DEV = 128
NB = 96
BANDS = 12
KFIRST = 8
CHUNK = 64
KMID, KSCALE = 0.13, 0.11 / 32700.0


def split(x):
    hi = x.astype(bf16)
    return hi, (x - hi.astype(f32)).astype(bf16)


def dot(a, b, ca, cb):
    return lax.dot_general(a, b, (((ca,), (cb,)), ((), ())), preferred_element_type=f32)


def iota(shape, dim):
    return lax.broadcasted_iota(i32, shape, dim)


def apart_matrix():
    target = (iota((256, 256), 1) & 127) * 2 + (iota((256, 256), 1) >> 7)
    return jnp.where(iota((256, 256), 0) == target, 1.0, 0.0).astype(bf16)


def kernel(
    traj_ref, kap_ref, end_ref, jac_ref, val_ref, wgt_ref, vld_ref, own_ref, til_ref,
    OR,
    TRJ, KIN, KQ, EIN, EQ, JAC,
    AS, AR, TT, LOH, ACC, BS, BR, S3, PR, CS, CR, RT, OHR,
    KS, KR, ES, EN, W, WT, KF, FB, OS,
    lsem, asem, bsem, csem, ksem, esem, fsem, osem,
):
    tm = lax.axis_index("tm")
    lat = lax.axis_index("lat")
    me = tm * 16 + lat
    half = lax.rem(tm, 2)
    pair = lax.div(tm, 2)
    level = pair * 16 + lat
    mate = tm + 1 - 2 * half
    side = lax.div(lat, 8)
    home = side == half
    away = side != half

    def peers(fn):
        def step(i, carry):
            d = lax.rem(me + i, DEV)
            fn(d, lax.div(d, 16), lax.rem(d, 16))
            return carry

        lax.fori_loop(1, DEV, step, 0, unroll=4)

    def send(src, dst, sems, t, l):
        return pltpu.make_async_remote_copy(
            src, dst, sems.at[0], sems.at[1], device_id=(t, l), device_id_type=MESH
        )

    def wait_n(buf, n, sem):
        part = buf.at[pl.ds(0, n)]
        pltpu.make_async_copy(part, part, sem).wait()

    def wait_home(buf, n, sem):
        @pl.when(home)
        def _():
            wait_n(buf, n - 1, sem)

        @pl.when(away)
        def _():
            wait_n(buf, n, sem)

    loads = [
        pltpu.make_async_copy(kap_ref, KIN, lsem.at[0]),
        pltpu.make_async_copy(
            end_ref.at[:, pl.ds(pl.multiple_of(pair * 16, 16), 16), :], EIN, lsem.at[1]
        ),
        pltpu.make_async_copy(traj_ref, TRJ, lsem.at[2]),
        pltpu.make_async_copy(jac_ref, JAC, lsem.at[3]),
    ]
    for copy in loads:
        copy.start()
    barrier = pltpu.get_barrier_semaphore()
    peers(
        lambda d, t, l: pl.semaphore_signal(barrier, 1, device_id=(t, l), device_id_type=MESH)
    )

    eye = iota((NB, NB), 0) == iota((NB, NB), 1)
    own_row = own_ref[...].astype(f32)
    own = jnp.sum(jnp.where(eye, own_row, 0.0), axis=1, keepdims=True)
    til = jnp.sum(jnp.where(eye, til_ref[...].astype(f32), 0.0), axis=1, keepdims=True)
    same = (own == own_row) & (iota((NB, NB), 1) < iota((NB, NB), 0))
    rank = jnp.sum(jnp.where(same, 1.0, 0.0), axis=1, keepdims=True)
    hit = iota((NB, 2 * DEV), 1) == (rank * DEV + own).astype(i32)
    M = jnp.where(hit, 1.0, 0.0).astype(bf16)
    ids = jnp.sum(jnp.where(hit, til + 1.0, 0.0), axis=0, keepdims=True)
    AS[0, 0:1, :] = ids[:, :DEV]
    AS[0, 1:2, :] = ids[:, DEV:]
    AR[me] = AS[0]

    pl.semaphore_wait(barrier, DEV - 1)
    peers(lambda d, t, l: send(AS.at[0], AR.at[me], asem, t, l).start())

    apart = apart_matrix()

    loads[0].wait()

    def kap_row(r, carry):
        for g in range(8):
            q = jnp.round((KIN[r, :, g * 256 : (g + 1) * 256] - KMID) * (1.0 / KSCALE))
            a = jnp.round(q * (1.0 / 256.0))
            b = q - a * 256.0
            y = dot(jnp.concatenate([a, b], axis=0).astype(bf16), apart, 1, 0)
            y = y[:64] * 256.0 + y[64:]
            rows = pl.ds(pl.multiple_of(r * 64, 64), 64)
            KQ[g, rows, :] = y[:, :128]
            KQ[8 + g, rows, :] = y[:, 128:]
        return carry

    lax.fori_loop(0, 4, kap_row, 0)
    k2 = KQ.reshape(16 * 256, 128)

    def kap_level(l, carry):
        for r in range(4):
            q = k2[pl.ds(r * 64 + l, 16, stride=256), :]
            KS[l, r * 16 : (r + 1) * 16, :] = q.astype(i32).astype(i16)
        return carry

    lax.fori_loop(0, 64, kap_level, 0, unroll=2)

    lb_me = lat - 4 * side

    @pl.when(home)
    def _():
        KR[lb_me * 8 + tm] = KS[level]

    def send_k(lo, hi):
        def step(i, carry):
            l = lax.rem(level + i * 27, 64)

            @pl.when((i > 0) | away)
            def _():
                send(
                    KS.at[l], KR.at[lb_me * 8 + tm], ksem, lax.div(l, 16) * 2 + side, lax.rem(l, 16)
                ).start()

            return carry

        lax.fori_loop(lo, hi, step, 0)

    def send_e(i, carry):
        i = lax.rem(i + lat, 8)
        l = half * 8 + i

        @pl.when((l != lat) | away)
        def _():
            send(ES.at[i], EN.at[lb_me], esem, pair * 2 + side, l).start()

        return carry

    send_k(0, KFIRST)

    loads[1].wait()
    for r in range(4):
        for g in range(8):
            y = dot(EIN[r, :, g * 256 : (g + 1) * 256], apart, 1, 0)
            EQ[g, r * 16 : (r + 1) * 16, :] = y[:, :128]
            EQ[8 + g, r * 16 : (r + 1) * 16, :] = y[:, 128:]
    e2 = EQ.reshape(16 * 64, 128)

    def end_level(l, carry):
        for r in range(4):
            rows = e2[pl.ds(r * 16 + half * 8 + l, 16, stride=64), :]
            ES[l, r * 16 : (r + 1) * 16, :] = rows.astype(bf16)
        return carry

    lax.fori_loop(0, 8, end_level, 0)

    @pl.when(home)
    def _():
        EN[lb_me] = ES[lat - 8 * half]

    lax.fori_loop(0, 8, send_e, 0)
    S3[...] = jnp.zeros((NB, 8, 128), f32)

    wait_n(AR, DEV - 1, asem.at[1])
    for s in range(2):
        TT[s] = AR[:, s, :].T
    tid = jnp.concatenate([TT[s, pl.ds(me, 1), :] for s in range(2)], axis=1).astype(i32) - 1
    low = (tid & 127) * 2
    group = jnp.concatenate([tid >> 7, tid >> 7], axis=1)
    LOH[...] = jnp.where(
        iota((256, 512), 0) == jnp.concatenate([low, low + 1], axis=1), 1.0, 0.0
    ).astype(bf16)
    ACC[...] = jnp.zeros((64, 512), f32)
    loads[2].wait()

    def gather_row(r, carry):
        total = ACC[...]
        for g in range(8):
            hi, lo = split(TRJ[r, :, g * 256 : (g + 1) * 256])
            y = dot(jnp.concatenate([hi, lo], axis=0), LOH[...], 1, 0)
            total = total + jnp.where(group == r * 8 + g, y[:64] + y[64:], 0.0)
        ACC[...] = total
        return carry

    lax.fori_loop(0, 4, gather_row, 0)
    for s in range(2):
        x = jnp.concatenate(
            [ACC[:, s * 128 : (s + 1) * 128], ACC[:, 256 + s * 128 : 256 + (s + 1) * 128]], axis=0
        )
        BS[:, s, :] = x.T
    BR[me] = BS[me]
    peers(lambda d, t, l: send(BS.at[d], BR.at[me], bsem, t, l).start())
    send_k(KFIRST, 64)


    def place(i, carry):
        o = lax.div(i, BANDS) * 16 + lax.rem(i, BANDS) + 4 * half
        t = jnp.concatenate([TT[k, pl.ds(o, 1), :] for k in range(2)], axis=1).astype(i32) - 1
        OHR[i] = jnp.where(iota((128, 256), 0) == (t & 127), 1.0, 0.0).astype(bf16)
        return carry

    lax.fori_loop(0, 8 * BANDS, place, 0)

    swap = jnp.where(
        iota((128, 128), 1) == (iota((128, 128), 0) & 63) * 2 + (iota((128, 128), 0) >> 6), 1.0, 0.0
    ).astype(bf16)
    weight = wgt_ref[...] * vld_ref[...].astype(f32)
    loads[3].wait()
    wait_n(BR, DEV - 1, bsem.at[1])
    parts = [split(BR[:, s, :]) for s in range(2)]
    for p in range(2):
        mine = dot(M[:, :DEV], parts[0][p], 1, 0) + dot(M[:, DEV:], parts[1][p], 1, 0)
        S3[:, p, :] = dot(mine.astype(bf16), swap, 1, 0)

    def predict(b, carry):
        PR[b] = dot(S3[b].astype(bf16), JAC[b], 1, 1)
        return carry

    lax.fori_loop(0, NB, predict, 0, unroll=32)
    resid = weight * (val_ref[...] - (PR[:, 0, :] + PR[:, 1, :]))
    for p, part in enumerate(split(resid)):
        S3[:, p, :] = part.astype(f32)

    def adjoin(b, carry):
        PR[b] = dot(S3[b].astype(bf16), JAC[b], 1, 0)
        return carry

    lax.fori_loop(0, NB, adjoin, 0, unroll=32)
    placed = jnp.zeros((128, 256), f32)
    for part in split(PR[:, 0, :] + PR[:, 1, :]):
        placed = placed + dot(dot(part, swap, 1, 1).astype(bf16), M, 0, 0)
    for s in range(2):
        for w in range(2):
            CS[:, s * 2 + w, :] = placed[w * 64 : (w + 1) * 64, s * 128 : (s + 1) * 128]
    CR[me] = CS[level]
    peers(lambda d, t, l: send(CS.at[lax.div(t, 2) * 16 + l], CR.at[me], csem, t, l).start())

    wait_home(KR, 64, ksem.at[1])
    wait_home(EN, 8, esem.at[1])
    halo_k = send(KR.at[pl.ds(32, 32)], KR.at[pl.ds(64 * half, 32)], fsem.at[0], mate, lat)
    halo_e = send(EN.at[pl.ds(4, 4)], EN.at[pl.ds(8 * half, 4)], fsem.at[1], mate, lat)
    halo_k.start()
    halo_e.start()
    halo_e.wait()
    for lb in range(BANDS):
        W[lb * 4 : lb * 4 + 4] = EN[lb].astype(f32).reshape(4, 16, 128)
    WT[0] = jnp.zeros((16, 128), f32)
    WT[49] = jnp.zeros((16, 128), f32)
    lane = iota((4, 8, 128), 2)
    halo_k.wait()

    def substeps(s):
        for step in range(2):
            for lb in range(BANDS):
                rows = slice(lb * 4, lb * 4 + 4)
                if step == 0:
                    k = KR[lb * 8 + s].astype(i32).astype(f32) * KSCALE + KMID
                    k = k.reshape(4, 16, 128)
                    KF[rows] = k
                else:
                    k = KF[rows]
                WT[1 + lb * 4 : 5 + lb * 4] = k * W[rows]
            for lb in range(BANDS):
                rows = slice(lb * 4, lb * 4 + 4)
                x = WT[1 + lb * 4 : 5 + lb * 4]
                even, odd = x[:, :8], x[:, 8:]
                a = pltpu.roll(odd, 1, axis=2)
                b = pltpu.roll(even, 127, axis=2)
                a = jnp.where(lane == 0, pltpu.roll(a, 1, axis=1), a)
                b = jnp.where(lane == 127, pltpu.roll(b, 7, axis=1), b)
                ends = WT[2 + lb * 4 : 6 + lb * 4] + WT[lb * 4 : lb * 4 + 4]
                w = W[rows]
                W[rows, :8] = w[:, :8] + (ends[:, :8] + (odd + a) - 4.0 * even)
                W[rows, 8:] = w[:, 8:] + (ends[:, 8:] + (even + b) - 4.0 * odd)

    def force(s):
        for lb in range(BANDS):
            o = s * 16 + lb + 4 * half
            t = jnp.concatenate([TT[k, pl.ds(o, 1), :] for k in range(2)], axis=1).astype(i32) - 1
            mask = iota((32, 256), 0) == (t >> 7)
            terms = []
            for w in range(2):
                term = jnp.concatenate([RT[k * 2 + w, pl.ds(o, 1), :] for k in range(2)], axis=1)
                terms.append(split(term))
            lhs = jnp.concatenate(
                [jnp.where(mask, terms[w][p].astype(f32), 0.0) for p in range(2) for w in range(2)],
                axis=0,
            ).astype(bf16)
            y = dot(lhs, OHR[s * BANDS + lb], 1, 1)
            y = y[:64] + y[64:]
            rows = slice(lb * 4, lb * 4 + 4)
            for w in range(2):
                part = slice(w * 8, w * 8 + 8)
                FB[rows, part] = y[w * 32 : w * 32 + 32].reshape(4, 8, 128)

    def finish(s):
        for lb in range(BANDS):
            rows = slice(lb * 4, lb * 4 + 4)
            W[rows] = W[rows] + FB[rows]

        for j in range(8):
            rows = W[pl.ds(half * 16 + j * 4, 4)]
            OS[s * 8 + j] = rows.reshape(CHUNK, 128).astype(bf16)

    def deliver(s, j):
        here = (s == tm) & (half * 8 + j == lat)

        @pl.when(jnp.logical_not(here))
        def _():
            send(OS.at[s * 8 + j], OR.at[level], osem, s, half * 8 + j).start()

    def deliver_early(s):
        def step(i, carry):
            deliver(s, lax.rem(i + lat + pair * 2, 8))
            return carry

        lax.fori_loop(0, 8, step, 0)

    def deliver_late(i, carry):
        q = lax.rem(i, 5)
        s = jnp.int32(0)
        for k, v in enumerate([0, 2, 4, 6, 1]):
            s = jnp.where(q == k, v, s)
        deliver(s, lax.rem(lax.div(i, 5) + lat + pair * 2 + q, 8))
        return carry

    substeps(7)
    wait_n(CR, DEV - 1, csem.at[1])
    for q in range(4):
        RT[q] = CR[:, q, :].T
    force(7)

    def section(i, carry):
        s = 7 - i
        finish(s)

        @pl.when((s == 7) | (s == 5) | (s == 3))
        def _():
            deliver_early(s)

        W[...] = W[...].astype(bf16).astype(f32)
        force(s - 1)
        substeps(s - 1)
        return carry

    lax.fori_loop(0, 7, section, 0)
    finish(0)
    lax.fori_loop(0, 40, deliver_late, 0)

    @pl.when(home)
    def _():
        OR[level] = OS[tm * 8 + lat - half * 8]

    wait_home(OR, 64, osem.at[1])

    wait_n(AR, DEV - 1, asem.at[0])
    wait_n(BS, DEV - 1, bsem.at[0])
    wait_n(CR, DEV - 1, csem.at[0])
    wait_home(ES, 8, esem.at[0])
    wait_home(KS, 64, ksem.at[0])
    wait_home(OS, 64, osem.at[0])


def decode(or_ref, out_ref, wide, rows, sem):
    apart = apart_matrix()

    def widen(l, carry):
        wide[pl.ds(pl.multiple_of(l * 64, 64), 64), :] = or_ref[l].astype(f32)
        return carry

    lax.fori_loop(0, 64, widen, 0, unroll=4)

    def copy(r):
        return pltpu.make_async_copy(rows.at[r], out_ref.at[r], sem.at[r])

    for r in range(4):
        for g in range(8):
            x = jnp.concatenate(
                [wide[pl.ds(r * 16 + w * 8 + g, 64, stride=64), :] for w in range(2)], axis=1
            )
            rows[r, :, g * 256 : (g + 1) * 256] = dot(x.astype(bf16), apart, 1, 1)
        copy(r).start()
    for r in range(4):
        copy(r).wait()


def per_device(traj, kap, end, jac, val, wgt, vld, own, til):
    hbm = pl.BlockSpec(memory_space=pl.ANY)
    vmem = pl.BlockSpec(memory_space=pltpu.VMEM)
    dma = pltpu.SemaphoreType.DMA
    V = pltpu.VMEM
    out = pl.pallas_call(
        kernel,
        out_shape=jax.ShapeDtypeStruct((64, CHUNK, 128), bf16),
        in_specs=[hbm] * 4 + [vmem] * 5,
        out_specs=vmem,
        scratch_shapes=[
            V((4, 64, 2048), f32), V((4, 64, 2048), f32), V((16, 256, 128), f32),
            V((4, 16, 2048), bf16), V((16, 64, 128), f32), V((NB, 128, 128), bf16),
            V((1, 2, 128), f32), V((DEV, 2, 128), f32), V((2, 128, 128), f32),
            V((256, 512), bf16), V((64, 512), f32), V((DEV, 2, 128), f32), V((DEV, 2, 128), f32),
            V((NB, 8, 128), f32), V((NB, 8, 128), f32), V((64, 4, 128), f32), V((DEV, 4, 128), f32),
            V((4, 128, 128), f32), V((8 * BANDS, 128, 256), bf16),
            V((64, CHUNK, 128), i16), V((8 * BANDS, CHUNK, 128), i16),
            V((8, CHUNK, 128), bf16), V((BANDS, CHUNK, 128), bf16),
            V((48, 16, 128), f32), V((50, 16, 128), f32), V((48, 16, 128), f32), V((48, 16, 128), f32),
            V((64, CHUNK, 128), bf16),
            dma((4,)), dma((2,)), dma((2,)), dma((2,)), dma((2,)), dma((2,)), dma((2, 2)), dma((2,)),
        ],
        compiler_params=pltpu.CompilerParams(
            has_side_effects=True, vmem_limit_bytes=56 << 20, collective_id=0
        ),
        name="adjoint_sweep",
    )(traj[0], kap[0], end, jac, val, wgt, vld, own.reshape(1, NB), til.reshape(1, NB))
    out = pl.pallas_call(
        decode,
        out_shape=jax.ShapeDtypeStruct((4, 64, 2048), f32),
        in_specs=[vmem],
        out_specs=hbm,
        scratch_shapes=[V((4096, 128), f32), V((4, 64, 2048), f32), dma((4,))],
        name="adjoint_decode",
    )(out)
    return out[None]


def solution(mesh):
    both = ("tm", "lat")
    in_specs = (
        P("tm", "lat", None, None),
        P("tm", "lat", None, None),
        P("lat", None, None),
        P(both, None, None),
        P(both, None),
        P(both, None),
        P(both, None),
        P(both, None),
        P(both),
    )
    return jax.shard_map(
        per_device, mesh=mesh, in_specs=in_specs, out_specs=P("tm", "lat", None, None),
        check_vma=False,
    )
```

```python
import jax
import jax.numpy as jnp
from jax import lax
from jax.experimental import pallas as pl
from jax.experimental.pallas import tpu as pltpu
from jax.sharding import PartitionSpec as P

f32, bf16, i16, i32 = jnp.float32, jnp.bfloat16, jnp.int16, jnp.int32
MESH = pl.DeviceIdType.MESH

DEV = 128
NB = 96
BANDS = 12
KFIRST = 8
CHUNK = 64
KMID, KSCALE = 0.13, 0.11 / 32700.0


def split(x):
    hi = x.astype(bf16)
    return hi, (x - hi.astype(f32)).astype(bf16)


def dot(a, b, ca, cb):
    return lax.dot_general(a, b, (((ca,), (cb,)), ((), ())), preferred_element_type=f32)


def iota(shape, dim):
    return lax.broadcasted_iota(i32, shape, dim)


def apart_matrix():
    target = (iota((256, 256), 1) & 127) * 2 + (iota((256, 256), 1) >> 7)
    return jnp.where(iota((256, 256), 0) == target, 1.0, 0.0).astype(bf16)


def kernel(
    traj_ref, kap_ref, end_ref, jac_ref, val_ref, wgt_ref, vld_ref, own_ref, til_ref,
    OR,
    TRJ, KIN, KQ, EIN, EQ, JAC,
    AS, AR, TT, LOH, ACC, BS, BR, MX, S3, S4, PR, CS, CR, RT, OHR,
    KS, KR, ES, EN, W, WT, KF, FB, OS,
    lsem, asem, bsem, csem, ksem, esem, fsem, osem,
):
    tm = lax.axis_index("tm")
    lat = lax.axis_index("lat")
    me = tm * 16 + lat
    half = lax.rem(tm, 2)
    pair = lax.div(tm, 2)
    level = pair * 16 + lat
    mate = tm + 1 - 2 * half
    side = lax.div(lat, 8)
    home = side == half
    away = side != half

    def peers(fn):
        def step(i, carry):
            d = lax.rem(me + i, DEV)
            fn(d, lax.div(d, 16), lax.rem(d, 16))
            return carry

        lax.fori_loop(1, DEV, step, 0, unroll=4)

    def send(src, dst, sems, t, l):
        return pltpu.make_async_remote_copy(
            src, dst, sems.at[0], sems.at[1], device_id=(t, l), device_id_type=MESH
        )

    def wait_n(buf, n, sem):
        part = buf.at[pl.ds(0, n)]
        pltpu.make_async_copy(part, part, sem).wait()

    def wait_home(buf, n, sem):
        @pl.when(home)
        def _():
            wait_n(buf, n - 1, sem)

        @pl.when(away)
        def _():
            wait_n(buf, n, sem)

    loads = [
        pltpu.make_async_copy(kap_ref, KIN, lsem.at[0]),
        pltpu.make_async_copy(
            end_ref.at[:, pl.ds(pl.multiple_of(pair * 16, 16), 16), :], EIN, lsem.at[1]
        ),
        pltpu.make_async_copy(traj_ref, TRJ, lsem.at[2]),
        pltpu.make_async_copy(jac_ref, JAC, lsem.at[3]),
    ]
    for copy in loads:
        copy.start()
    barrier = pltpu.get_barrier_semaphore()
    peers(
        lambda d, t, l: pl.semaphore_signal(barrier, 1, device_id=(t, l), device_id_type=MESH)
    )

    eye = iota((NB, NB), 0) == iota((NB, NB), 1)
    own_row = own_ref[...].astype(f32)
    own = jnp.sum(jnp.where(eye, own_row, 0.0), axis=1, keepdims=True)
    til = jnp.sum(jnp.where(eye, til_ref[...].astype(f32), 0.0), axis=1, keepdims=True)
    same = (own == own_row) & (iota((NB, NB), 1) < iota((NB, NB), 0))
    rank = jnp.sum(jnp.where(same, 1.0, 0.0), axis=1, keepdims=True)
    hit = iota((NB, 2 * DEV), 1) == (rank * DEV + own).astype(i32)
    M = jnp.where(hit, 1.0, 0.0).astype(bf16)
    ids = jnp.sum(jnp.where(hit, til + 1.0, 0.0), axis=0, keepdims=True)
    AS[0, 0:1, :] = ids[:, :DEV]
    AS[0, 1:2, :] = ids[:, DEV:]
    AR[me] = AS[0]

    pl.semaphore_wait(barrier, DEV - 1)
    peers(lambda d, t, l: send(AS.at[0], AR.at[me], asem, t, l).start())

    apart = apart_matrix()

    loads[0].wait()

    def kap_row(r, carry):
        for g in range(8):
            q = jnp.round((KIN[r, :, g * 256 : (g + 1) * 256] - KMID) * (1.0 / KSCALE))
            a = jnp.round(q * (1.0 / 256.0))
            b = q - a * 256.0
            y = dot(jnp.concatenate([a, b], axis=0).astype(bf16), apart, 1, 0)
            y = y[:64] * 256.0 + y[64:]
            rows = pl.ds(pl.multiple_of(r * 64, 64), 64)
            KQ[g, rows, :] = y[:, :128]
            KQ[8 + g, rows, :] = y[:, 128:]
        return carry

    lax.fori_loop(0, 4, kap_row, 0)
    k2 = KQ.reshape(16 * 256, 128)

    def kap_level(l, carry):
        for r in range(4):
            q = k2[pl.ds(r * 64 + l, 16, stride=256), :]
            KS[l, r * 16 : (r + 1) * 16, :] = q.astype(i32).astype(i16)
        return carry

    lax.fori_loop(0, 64, kap_level, 0, unroll=2)

    lb_me = lat - 4 * side

    @pl.when(home)
    def _():
        KR[lb_me * 8 + tm] = KS[level]

    def send_k(lo, hi):
        def step(i, carry):
            l = lax.rem(level + i * 27, 64)

            @pl.when((i > 0) | away)
            def _():
                send(
                    KS.at[l], KR.at[lb_me * 8 + tm], ksem, lax.div(l, 16) * 2 + side, lax.rem(l, 16)
                ).start()

            return carry

        lax.fori_loop(lo, hi, step, 0)

    def send_e(i, carry):
        i = lax.rem(i + lat, 8)
        l = half * 8 + i

        @pl.when((l != lat) | away)
        def _():
            send(ES.at[i], EN.at[lb_me], esem, pair * 2 + side, l).start()

        return carry

    send_k(0, KFIRST)

    loads[1].wait()
    for r in range(4):
        for g in range(8):
            y = dot(EIN[r, :, g * 256 : (g + 1) * 256], apart, 1, 0)
            EQ[g, r * 16 : (r + 1) * 16, :] = y[:, :128]
            EQ[8 + g, r * 16 : (r + 1) * 16, :] = y[:, 128:]
    e2 = EQ.reshape(16 * 64, 128)

    def end_level(l, carry):
        for r in range(4):
            rows = e2[pl.ds(r * 16 + half * 8 + l, 16, stride=64), :]
            ES[l, r * 16 : (r + 1) * 16, :] = rows.astype(bf16)
        return carry

    lax.fori_loop(0, 8, end_level, 0)

    @pl.when(home)
    def _():
        EN[lb_me] = ES[lat - 8 * half]

    lax.fori_loop(0, 8, send_e, 0)
    S3[...] = jnp.zeros((NB // 2, 8, 128), f32)
    S4[...] = jnp.zeros((NB // 2, 8, 256), f32)

    wait_n(AR, DEV - 1, asem.at[1])
    for s in range(2):
        TT[s] = AR[:, s, :].T
    tid = jnp.concatenate([TT[s, pl.ds(me, 1), :] for s in range(2)], axis=1).astype(i32) - 1
    low = (tid & 127) * 2
    group = jnp.concatenate([tid >> 7, tid >> 7], axis=1)
    LOH[...] = jnp.where(
        iota((256, 512), 0) == jnp.concatenate([low, low + 1], axis=1), 1.0, 0.0
    ).astype(bf16)
    ACC[...] = jnp.zeros((64, 512), f32)
    loads[2].wait()

    def gather_row(r, carry):
        total = ACC[...]
        for g in range(8):
            hi, lo = split(TRJ[r, :, g * 256 : (g + 1) * 256])
            y = dot(jnp.concatenate([hi, lo], axis=0), LOH[...], 1, 0)
            total = total + jnp.where(group == r * 8 + g, y[:64] + y[64:], 0.0)
        ACC[...] = total
        return carry

    lax.fori_loop(0, 4, gather_row, 0)
    for s in range(2):
        x = jnp.concatenate(
            [ACC[:, s * 128 : (s + 1) * 128], ACC[:, 256 + s * 128 : 256 + (s + 1) * 128]], axis=0
        )
        BS[:, s, :] = x.T
    BR[me] = BS[me]
    peers(lambda d, t, l: send(BS.at[d], BR.at[me], bsem, t, l).start())
    send_k(KFIRST, 64)


    def place(i, carry):
        o = lax.div(i, BANDS) * 16 + lax.rem(i, BANDS) + 4 * half
        t = jnp.concatenate([TT[k, pl.ds(o, 1), :] for k in range(2)], axis=1).astype(i32) - 1
        OHR[i] = jnp.where(iota((128, 256), 0) == (t & 127), 1.0, 0.0).astype(bf16)
        return carry

    lax.fori_loop(0, 8 * BANDS, place, 0)

    swap = jnp.where(
        iota((128, 128), 1) == (iota((128, 128), 0) & 63) * 2 + (iota((128, 128), 0) >> 6), 1.0, 0.0
    ).astype(bf16)
    loads[3].wait()
    wait_n(BR, DEV - 1, bsem.at[1])
    parts = [split(BR[:, s, :]) for s in range(2)]
    for p in range(2):
        mine = dot(M[:, :DEV], parts[0][p], 1, 0) + dot(M[:, DEV:], parts[1][p], 1, 0)
        MX[p] = dot(mine.astype(bf16), swap, 1, 0)
    pairs = JAC.reshape(NB // 2, 256, 128)
    for q in range(2):
        for p in range(2):
            S3[:, q * 2 + p, :] = MX[p, pl.ds(q, NB // 2, stride=2), :]

    def predict(k, carry):
        PR[k] = dot(S3[k].astype(bf16), pairs[k], 1, 1)
        return carry

    lax.fori_loop(0, NB // 2, predict, 0, unroll=16)
    for q in range(2):
        rows, cols = pl.ds(q, NB // 2, stride=2), slice(q * 128, q * 128 + 128)
        weight = wgt_ref[rows, :] * vld_ref[rows, :].astype(f32)
        pred = PR[:, q * 2, cols] + PR[:, q * 2 + 1, cols]
        for p, part in enumerate(split(weight * (val_ref[rows, :] - pred))):
            S4[:, q * 2 + p, cols] = part.astype(f32)

    def adjoin(k, carry):
        S3[k] = dot(S4[k].astype(bf16), pairs[k], 1, 0)
        return carry

    lax.fori_loop(0, NB // 2, adjoin, 0, unroll=16)
    for q in range(2):
        MX[0, pl.ds(q, NB // 2, stride=2), :] = S3[:, q * 2, :] + S3[:, q * 2 + 1, :]
    placed = jnp.zeros((128, 256), f32)
    for part in split(MX[0]):
        placed = placed + dot(dot(part, swap, 1, 1).astype(bf16), M, 0, 0)
    for s in range(2):
        for w in range(2):
            CS[:, s * 2 + w, :] = placed[w * 64 : (w + 1) * 64, s * 128 : (s + 1) * 128]
    CR[me] = CS[level]
    peers(lambda d, t, l: send(CS.at[lax.div(t, 2) * 16 + l], CR.at[me], csem, t, l).start())

    wait_home(KR, 64, ksem.at[1])
    wait_home(EN, 8, esem.at[1])
    halo_k = send(KR.at[pl.ds(32, 32)], KR.at[pl.ds(64 * half, 32)], fsem.at[0], mate, lat)
    halo_e = send(EN.at[pl.ds(4, 4)], EN.at[pl.ds(8 * half, 4)], fsem.at[1], mate, lat)
    halo_k.start()
    halo_e.start()
    halo_e.wait()
    for lb in range(BANDS):
        W[lb * 4 : lb * 4 + 4] = EN[lb].astype(f32).reshape(4, 16, 128)
    WT[0] = jnp.zeros((16, 128), f32)
    WT[49] = jnp.zeros((16, 128), f32)
    lane = iota((4, 8, 128), 2)
    halo_k.wait()

    def substeps(s):
        for step in range(2):
            for lb in range(BANDS):
                rows = slice(lb * 4, lb * 4 + 4)
                if step == 0:
                    k = KR[lb * 8 + s].astype(i32).astype(f32) * KSCALE + KMID
                    k = k.reshape(4, 16, 128)
                    KF[rows] = k
                else:
                    k = KF[rows]
                WT[1 + lb * 4 : 5 + lb * 4] = k * W[rows]
            for lb in range(BANDS):
                rows = slice(lb * 4, lb * 4 + 4)
                x = WT[1 + lb * 4 : 5 + lb * 4]
                even, odd = x[:, :8], x[:, 8:]
                a = pltpu.roll(odd, 1, axis=2)
                b = pltpu.roll(even, 127, axis=2)
                a = jnp.where(lane == 0, pltpu.roll(a, 1, axis=1), a)
                b = jnp.where(lane == 127, pltpu.roll(b, 7, axis=1), b)
                ends = WT[2 + lb * 4 : 6 + lb * 4] + WT[lb * 4 : lb * 4 + 4]
                w = W[rows]
                W[rows, :8] = w[:, :8] + (ends[:, :8] + (odd + a) - 4.0 * even)
                W[rows, 8:] = w[:, 8:] + (ends[:, 8:] + (even + b) - 4.0 * odd)

    def force(s):
        for lb in range(BANDS):
            o = s * 16 + lb + 4 * half
            t = jnp.concatenate([TT[k, pl.ds(o, 1), :] for k in range(2)], axis=1).astype(i32) - 1
            mask = iota((32, 256), 0) == (t >> 7)
            terms = []
            for w in range(2):
                term = jnp.concatenate([RT[k * 2 + w, pl.ds(o, 1), :] for k in range(2)], axis=1)
                terms.append(split(term))
            lhs = jnp.concatenate(
                [jnp.where(mask, terms[w][p].astype(f32), 0.0) for p in range(2) for w in range(2)],
                axis=0,
            ).astype(bf16)
            y = dot(lhs, OHR[s * BANDS + lb], 1, 1)
            y = y[:64] + y[64:]
            rows = slice(lb * 4, lb * 4 + 4)
            for w in range(2):
                part = slice(w * 8, w * 8 + 8)
                FB[rows, part] = y[w * 32 : w * 32 + 32].reshape(4, 8, 128)

    def finish(s):
        for lb in range(BANDS):
            rows = slice(lb * 4, lb * 4 + 4)
            W[rows] = W[rows] + FB[rows]

        for j in range(8):
            rows = W[pl.ds(half * 16 + j * 4, 4)]
            OS[s * 8 + j] = rows.reshape(CHUNK, 128).astype(bf16)

    def deliver(s, j):
        here = (s == tm) & (half * 8 + j == lat)

        @pl.when(jnp.logical_not(here))
        def _():
            send(OS.at[s * 8 + j], OR.at[level], osem, s, half * 8 + j).start()

    def deliver_early(s):
        def step(i, carry):
            deliver(s, lax.rem(i + lat + pair * 2, 8))
            return carry

        lax.fori_loop(0, 8, step, 0)

    def deliver_late(i, carry):
        q = lax.rem(i, 5)
        s = jnp.int32(0)
        for k, v in enumerate([0, 2, 4, 6, 1]):
            s = jnp.where(q == k, v, s)
        deliver(s, lax.rem(lax.div(i, 5) + lat + pair * 2 + q, 8))
        return carry

    substeps(7)
    wait_n(CR, DEV - 1, csem.at[1])
    for q in range(4):
        RT[q] = CR[:, q, :].T
    force(7)

    def section(i, carry):
        s = 7 - i
        finish(s)

        @pl.when((s == 7) | (s == 5) | (s == 3))
        def _():
            deliver_early(s)

        W[...] = W[...].astype(bf16).astype(f32)
        force(s - 1)
        substeps(s - 1)
        return carry

    lax.fori_loop(0, 7, section, 0)
    finish(0)
    lax.fori_loop(0, 40, deliver_late, 0, unroll=4)

    @pl.when(home)
    def _():
        OR[level] = OS[tm * 8 + lat - half * 8]

    wait_home(OR, 64, osem.at[1])

    wait_n(AR, DEV - 1, asem.at[0])
    wait_n(BS, DEV - 1, bsem.at[0])
    wait_n(CR, DEV - 1, csem.at[0])
    wait_home(ES, 8, esem.at[0])
    wait_home(KS, 64, ksem.at[0])
    wait_home(OS, 64, osem.at[0])


def decode(or_ref, out_ref, chunks, wide, rows, isem, osem):
    def load(r):
        return pltpu.make_async_copy(
            or_ref.at[:, pl.ds(r * 16, 16), :], chunks.at[r], isem.at[r]
        )

    def copy(r):
        return pltpu.make_async_copy(rows.at[r], out_ref.at[r], osem.at[r])

    for r in range(4):
        load(r).start()
    apart = apart_matrix()
    for r in range(4):
        load(r).wait()
        wide[r] = chunks[r].astype(f32).reshape(1024, 128)
        for g in range(8):
            x = jnp.concatenate(
                [wide[r, pl.ds(w * 8 + g, 64, stride=16), :] for w in range(2)], axis=1
            )
            rows[r, :, g * 256 : (g + 1) * 256] = dot(x.astype(bf16), apart, 1, 1)
        copy(r).start()
    for r in range(4):
        copy(r).wait()


def per_device(traj, kap, end, jac, val, wgt, vld, own, til):
    hbm = pl.BlockSpec(memory_space=pl.ANY)
    vmem = pl.BlockSpec(memory_space=pltpu.VMEM)
    dma = pltpu.SemaphoreType.DMA
    V = pltpu.VMEM
    out = pl.pallas_call(
        kernel,
        out_shape=jax.ShapeDtypeStruct((64, CHUNK, 128), bf16),
        in_specs=[hbm] * 4 + [vmem] * 5,
        out_specs=vmem,
        scratch_shapes=[
            V((4, 64, 2048), f32), V((4, 64, 2048), f32), V((16, 256, 128), f32),
            V((4, 16, 2048), bf16), V((16, 64, 128), f32), V((NB, 128, 128), bf16),
            V((1, 2, 128), f32), V((DEV, 2, 128), f32), V((2, 128, 128), f32),
            V((256, 512), bf16), V((64, 512), f32), V((DEV, 2, 128), f32), V((DEV, 2, 128), f32),
            V((2, NB, 128), f32), V((NB // 2, 8, 128), f32), V((NB // 2, 8, 256), f32),
            V((NB // 2, 8, 256), f32), V((64, 4, 128), f32), V((DEV, 4, 128), f32),
            V((4, 128, 128), f32), V((8 * BANDS, 128, 256), bf16),
            V((64, CHUNK, 128), i16), V((8 * BANDS, CHUNK, 128), i16),
            V((8, CHUNK, 128), bf16), V((BANDS, CHUNK, 128), bf16),
            V((48, 16, 128), f32), V((50, 16, 128), f32), V((48, 16, 128), f32), V((48, 16, 128), f32),
            V((64, CHUNK, 128), bf16),
            dma((4,)), dma((2,)), dma((2,)), dma((2,)), dma((2,)), dma((2,)), dma((2, 2)), dma((2,)),
        ],
        compiler_params=pltpu.CompilerParams(
            has_side_effects=True, vmem_limit_bytes=56 << 20, collective_id=0
        ),
        name="adjoint_sweep",
    )(traj[0], kap[0], end, jac, val, wgt, vld, own.reshape(1, NB), til.reshape(1, NB))
    out = pl.pallas_call(
        decode,
        out_shape=jax.ShapeDtypeStruct((4, 64, 2048), f32),
        in_specs=[hbm],
        out_specs=hbm,
        scratch_shapes=[
            V((4, 64, 16, 128), bf16), V((4, 1024, 128), f32), V((4, 64, 2048), f32),
            dma((4,)), dma((4,)),
        ],
        name="adjoint_decode",
    )(out)
    return out[None]


def solution(mesh):
    both = ("tm", "lat")
    in_specs = (
        P("tm", "lat", None, None),
        P("tm", "lat", None, None),
        P("lat", None, None),
        P(both, None, None),
        P(both, None),
        P(both, None),
        P(both, None),
        P(both, None),
        P(both),
    )
    return jax.shard_map(
        per_device, mesh=mesh, in_specs=in_specs, out_specs=P("tm", "lat", None, None),
        check_vma=False,
    )
```
